8 devices in a mesh: m: 1 (over z), kk: 2 (over y), g: 4 (over x, core).
Axes of the slice: x: 2, y: 2, z: 1, core: 2. Of those that a mesh axis runs over, the one named last changes fastest.
Arguments:
- a_mat: bfloat16 [2, 8192, 28672], P(None, ('m', 'g'), 'kk')
Outputs:
- output: float32 [4, 3, 2, 2048, 2048], P(('m', 'g'))
All inputs are finite; a program needn't handle non-finite values.
Results may differ from the reference program's by a relative error of at most 0.001.
Values are sent between devices in bfloat16 or wider.
A program may use at most 1 GiB of HBM per device.

```python
import jax
import jax.numpy as jnp
from jax import lax

ROWS = 8192
COLS = 28672
LAYERS = 2
GROUP = 4

BLOCK = ROWS // GROUP
SLOTS = GROUP // 2 + 1


def assignment_table(groups):
    slot_count = groups // 2 + 1
    log_two = groups.bit_length() - 1
    side_len = 2 ** (log_two // 2)
    dup_count = groups // (side_len * side_len)
    grp_width = groups // side_len
    piece_len = max(1, grp_width // (2 * dup_count))
    pair_lists = [[] for device_no in range(groups)]
    block_sets = [set() for device_no in range(groups)]
    spill_pairs = []
    for upper_grp in range(side_len):
        for lower_grp in range(upper_grp):
            for left_row in range(upper_grp * grp_width, (upper_grp + 1) * grp_width):
                part_no = (left_row % grp_width) // piece_len
                if part_no < dup_count:
                    target = dup_count * (upper_grp * side_len + lower_grp) + part_no
                else:
                    target = dup_count * (lower_grp * side_len + upper_grp) + part_no - dup_count
                for right_row in range(lower_grp * grp_width, (lower_grp + 1) * grp_width):
                    pair_lists[target].append((left_row, right_row))
                    block_sets[target].update([left_row, right_row])
    for diag_grp in range(side_len):
        first_dev = dup_count * (diag_grp * side_len + diag_grp)
        for left_row in range(diag_grp * grp_width, (diag_grp + 1) * grp_width):
            for right_row in range(diag_grp * grp_width, left_row + 1):
                target = -1
                for copy_no in range(dup_count):
                    if target < 0 and len(pair_lists[first_dev + copy_no]) < slot_count:
                        target = first_dev + copy_no
                if target < 0:
                    spill_pairs.append((left_row, right_row))
                else:
                    pair_lists[target].append((left_row, right_row))
                    block_sets[target].update([left_row, right_row])
    for (left_row, right_row) in spill_pairs:
        best_score = (3, groups + 1, groups)
        for device_no in range(groups):
            if len(pair_lists[device_no]) < slot_count:
                growth = len(set([left_row, right_row]) - block_sets[device_no])
                cand_score = (growth, len(pair_lists[device_no]), device_no)
                best_score = min(best_score, cand_score)
        target = best_score[2]
        pair_lists[target].append((left_row, right_row))
        block_sets[target].update([left_row, right_row])
    return pair_lists, block_sets


def slot_tables(groups):
    pair_lists = assignment_table(groups)[0]
    slot_count = groups // 2 + 1
    left_rows = []
    right_rows = []
    live_flags = []
    for device_no in range(groups):
        own_pairs = pair_lists[device_no]
        left_rows.append([own_pairs[slot_no][0] if slot_no < len(own_pairs) else 0 for slot_no in range(slot_count)])
        right_rows.append([own_pairs[slot_no][1] if slot_no < len(own_pairs) else 0 for slot_no in range(slot_count)])
        live_flags.append([1 if slot_no < len(own_pairs) else 0 for slot_no in range(slot_count)])
    return left_rows, right_rows, live_flags


def setup_inputs(seed: int = 0, part: int = 0) -> dict:
    base_key = jax.random.fold_in(jax.random.key(seed), part)
    draw_key, scale_key = jax.random.split(base_key)
    values = jax.random.normal(draw_key, (LAYERS, GROUP, BLOCK, COLS), jnp.float32)
    block_scale = jnp.exp(jax.random.uniform(scale_key, (LAYERS, GROUP, 1, 1), jnp.float32, -0.35, 0.35))
    values = values * block_scale * (COLS ** -0.25)
    return {"a_mat": values.reshape(LAYERS, ROWS, COLS).astype(jnp.bfloat16)}


def reference(a_mat):
    left_rows, right_rows, live_flags = slot_tables(GROUP)

    def one_slot(slot_args):
        left_no, right_no, live_flag = slot_args
        left_blk = lax.dynamic_slice_in_dim(a_mat, left_no * BLOCK, BLOCK, axis=1).astype(jnp.float32)
        right_blk = lax.dynamic_slice_in_dim(a_mat, right_no * BLOCK, BLOCK, axis=1).astype(jnp.float32)
        product = jnp.einsum("lbk,lck->lbc", left_blk, right_blk)
        return jnp.where(live_flag == 1, product, jnp.zeros_like(product))

    blocks = lax.map(one_slot, (jnp.array(left_rows, jnp.int32).reshape(-1), jnp.array(right_rows, jnp.int32).reshape(-1), jnp.array(live_flags, jnp.int32).reshape(-1)))
    return blocks.reshape(GROUP, SLOTS, LAYERS, BLOCK, BLOCK)
```

```python
import jax
import jax.numpy as jnp
from jax import lax
from jax.experimental import pallas as pl
from jax.experimental.pallas import tpu as pltpu
from jax.sharding import PartitionSpec as P

MESH = pl.DeviceIdType.MESH
NT = (((1,), (1,)), ((), ()))
F32 = jnp.float32

TILE = 512
CHUNK = 128
STRIPS = 24
KSTEPS = 2


def kernel(a, out, blk, prv, awy, res, stm, acc, fa, fb, fc,
           s_x, r_x, s_d, r_d, s_y, r_y, s_r, r_r,
           l_res, l_stm, l_acc, l_fa, l_fb, l_st, l_tr):
    m = lax.axis_index("m")
    y = lax.axis_index("kk")
    g = lax.axis_index("g")
    side = lax.div(g, 2)
    layers, rows, cols = a.shape
    kc = cols // KSTEPS
    n_strip = rows // TILE
    n_chunk = rows // CHUNK

    def at(start, size):
        return pl.ds(pl.multiple_of(start, size), size)

    def remote(src, dst, ss, rs, kk2, g2):
        return pltpu.make_async_remote_copy(src, dst, ss, rs, device_id=(m, kk2, g2), device_id_type=MESH)

    barrier = pltpu.get_barrier_semaphore()
    me = y * 4 + g
    for step in range(1, 8):
        other = lax.rem(me + step, 8)
        pl.semaphore_signal(barrier, inc=1, device_id=(m, lax.div(other, 4), lax.rem(other, 4)), device_id_type=MESH)
    pl.semaphore_wait(barrier, 7)

    def x_in(c):
        part = lax.rem(g, 2)
        return remote(a.at[1 - side, at(c * CHUNK, CHUNK)], blk.at[1 + part, at(c * CHUNK, CHUNK)],
                      s_x.at[c], r_x.at[part, c], y, 2 - side)

    def x_start(c, carry):
        x_in(c).start()
        return carry

    def x_wait_send(c, carry):
        x_in(c).wait_send()
        return carry

    def body_steps(res_view, acc_view, swap, after):
        acc_view[...] = jnp.zeros(acc_view.shape, F32)

        def step(k, carry):
            pltpu.make_async_copy(a.at[0, pl.ds(0, TILE), pl.ds(0, kc)], stm.at[k], l_stm.at[k]).wait()
            lhs = res_view[:, at(k * kc, kc)]
            rhs = stm[k]
            if swap:
                lhs, rhs = rhs, lhs
            acc_view[...] += lax.dot_general(lhs, rhs, NT, preferred_element_type=F32)
            after(k)
            return carry

        lax.fori_loop(0, KSTEPS, step, 0)

    def diagonal():
        d = lax.div(g, 3)
        mate = g + 1 - 2 * d
        d2d = remote(a.at[side], blk.at[0], s_d.at[0], r_d.at[0], y, mate)
        d2d.start()
        lax.fori_loop(0, n_chunk, x_start, 0)

        def phase(r):
            return lax.div(r, 8), lax.rem(lax.div(r, 4), 2), lax.rem(r, 4)

        def count(r):
            p, _, i = phase(r)
            return (i + 1) + lax.rem(p, 2) * (n_strip - 1 - i)

        def slot(p):
            return p * (1 - 2 * d) + 2 * d

        def load(own, layer, row, col, width, dst, sem):
            @pl.when(own)
            def _():
                pltpu.make_async_copy(a.at[layer, at(row, TILE), at(col, width)], dst, sem).start()

            @pl.when(jnp.logical_not(own))
            def _():
                pltpu.make_async_copy(blk.at[layer, at(row, TILE), at(col, width)], dst, sem).start()

        def load_res(r):
            p, layer, i = phase(r)
            own = p + 1 - d < 2
            load(own, layer, i * TILE, 0, cols, res.at[lax.rem(r, 2)], l_res.at[lax.rem(r, 2)])

        def load_stm(r, j, k):
            p, layer, _ = phase(r)
            own = p + d < 2
            load(own, layer, j * TILE, k * kc, kc, stm.at[k], l_stm.at[k])

        def tile_of(ref, r, i, j):
            p, layer, _ = phase(r)
            return ref.at[slot(p), layer, at(i * TILE, TILE), at(j * TILE, TILE)]

        def is_diag(r, j):
            p, _, i = phase(r)
            return jnp.logical_and(p != 1, i == j)

        def is_mirror(r, j):
            p, _, i = phase(r)
            return jnp.logical_and(p != 1, i != j)

        def whole(r, j):
            i = lax.rem(r, 4)
            return remote(tile_of(out, r, i, j), tile_of(prv, r, i, j),
                          s_y.at[lax.rem(r, 4) * 4 + j], r_y.at[r * 4 + j], 1 - y, g)

        def lower(r, j, row, height, width):
            p, layer, i = phase(r)

            def part(ref):
                return ref.at[slot(p), layer, pl.ds(pl.multiple_of(i * TILE + row, 128), height), pl.ds(pl.multiple_of(j * TILE, TILE), width)]

            return remote(part(out), part(prv), s_y.at[lax.rem(r, 4) * 4 + j], r_y.at[r * 4 + j], 1 - y, g)

        def send(r, j):
            @pl.when(is_diag(r, j))
            def _():
                for q in range(4):
                    lower(r, j, q * 128, 128, (q + 1) * 128).start()

            @pl.when(jnp.logical_not(is_diag(r, j)))
            def _():
                whole(r, j).start()

        def wait_exchange(r, j):
            @pl.when(is_diag(r, j))
            def _():
                sized = lower(r, j, 0, 320, TILE)
                sized.wait_send()
                sized.wait_recv()

            @pl.when(jnp.logical_not(is_diag(r, j)))
            def _():
                whole(r, j).wait_send()
                whole(r, j).wait_recv()

        def store_acc(r, j):
            return pltpu.make_async_copy(acc.at[lax.rem(j, 2)], tile_of(out, r, lax.rem(r, 4), j), l_acc.at[lax.rem(j, 2)])

        def finish(r):
            n = count(r)
            i = lax.rem(r, 4)

            def loads(j):
                b = lax.rem(j, 2)
                return (pltpu.make_async_copy(tile_of(out, r, i, j), fa.at[b], l_fa.at[b]),
                        pltpu.make_async_copy(tile_of(prv, r, i, j), fb.at[b], l_fb.at[b]))

            def start_loads(j):
                wait_exchange(r, j)
                for copy in loads(j):
                    copy.start()

            def main_store(j):
                return pltpu.make_async_copy(fa.at[lax.rem(j, 2)], tile_of(out, r, i, j), l_st.at[lax.rem(j, 2)])

            def mirror_store(j):
                return pltpu.make_async_copy(fc.at[lax.rem(j, 2)], tile_of(out, r, j, i), l_tr.at[lax.rem(j, 2)])

            def wait_stores(j):
                main_store(j).wait()

                @pl.when(is_mirror(r, j))
                def _():
                    mirror_store(j).wait()

            start_loads(0)

            def one(j, carry):
                b = lax.rem(j, 2)

                @pl.when(j + 1 < n)
                def _():
                    @pl.when(j >= 1)
                    def _():
                        wait_stores(j - 1)

                    start_loads(j + 1)

                for copy in loads(j):
                    copy.wait()
                fa[b] = fa[b] + fb[b]

                @pl.when(is_mirror(r, j))
                def _():
                    fc[b] = fa[b].T
                    mirror_store(j).start()

                @pl.when(is_diag(r, j))
                def _():
                    total = fa[b]
                    at_row = lax.broadcasted_iota(jnp.int32, (TILE, TILE), 0)
                    at_col = lax.broadcasted_iota(jnp.int32, (TILE, TILE), 1)
                    fa[b] = jnp.where(at_row >= at_col, total, total.T)

                main_store(j).start()
                return carry

            lax.fori_loop(0, n, one, 0)

            @pl.when(n >= 2)
            def _():
                wait_stores(n - 2)

            wait_stores(n - 1)

        load_res(0)
        for k in range(KSTEPS):
            load_stm(0, 0, k)

        def strip(r, carry):
            @pl.when(r == 7)
            def _():
                remote(a.at[0], blk.at[0], s_d.at[0], r_d.at[0], y, mate).wait_recv()

            @pl.when(r == 11)
            def _():
                remote(a.at[1], blk.at[1], s_d.at[1], r_d.at[1], y, mate).wait_recv()

            @pl.when(r + 1 < STRIPS)
            def _():
                load_res(r + 1)

            pltpu.make_async_copy(a.at[0, pl.ds(0, TILE)], res.at[lax.rem(r, 2)], l_res.at[lax.rem(r, 2)]).wait()
            n = count(r)

            def tile(j, carry):
                last = lax.div(j + 1, n)

                def after(k):
                    @pl.when(r + last < STRIPS)
                    def _():
                        load_stm(r + last, (j + 1) * (1 - last), k)

                    @pl.when(jnp.logical_and(k == 0, j >= 1))
                    def _():
                        store_acc(r, j - 1).wait()
                        send(r, j - 1)

                body_steps(res.at[lax.rem(r, 2)], acc.at[lax.rem(j, 2)], False, after)
                store_acc(r, j).start()
                return carry

            lax.fori_loop(0, n, tile, 0)
            store_acc(r, n - 1).wait()
            send(r, n - 1)

            @pl.when(r >= 2)
            def _():
                finish(r - 2)

            return carry

        lax.fori_loop(0, STRIPS, strip, 0)
        lax.fori_loop(STRIPS - 2, STRIPS, lambda r, carry: (finish(r), carry)[1], 0)
        d2d.wait_send()
        lax.fori_loop(0, n_chunk, x_wait_send, 0)

    def cross(is_left):
        lc = 0 if is_left else 1
        mate = 0 if is_left else 3
        partner = 2 if is_left else 1
        for layer in range(layers):
            remote(a.at[layer], blk.at[layer], s_d.at[layer], r_d.at[layer], y, mate).start()
        lax.fori_loop(0, n_chunk, x_start, 0)

        fc[0] = jnp.zeros((TILE, TILE), F32)

        def zero(t, carry):
            copies = [pltpu.make_async_copy(fc.at[0], out.at[2, lax.div(t, 4), at(lax.rem(t, 4) * TILE, TILE), pl.ds(q * TILE, TILE)], l_fa.at[q])
                      for q in range(4)]
            for copy in copies:
                copy.start()
            for copy in copies:
                copy.wait()
            return carry

        lax.fori_loop(0, layers * n_strip, zero, 0)
        remote(a.at[lc], blk.at[0], s_d.at[0], r_d.at[0], y, mate).wait_recv()

        def region(ref, rows_first, c):
            return ref.at[at(c * CHUNK, CHUNK), :] if rows_first else ref.at[:, at(c * CHUNK, CHUNK)]

        def piece(ref, c, q):
            if is_left:
                return ref.at[at(c * CHUNK, CHUNK), at(q * TILE, TILE)]
            return ref.at[at(q * TILE, TILE), at(c * CHUNK, CHUNK)]

        def block_of(half):
            return lax.rem(half + 1 - y + 2, 2)

        def kept(b):
            return lax.rem(b + 1 - y + 2, 2)

        def load_stm(t, k):
            half, js = lax.div(t, 4), lax.rem(t, 4)
            own = block_of(half) == 1 if is_left else half == 1

            @pl.when(own)
            def _():
                pltpu.make_async_copy(a.at[lc, at(js * TILE, TILE), at(k * kc, kc)], stm.at[k], l_stm.at[k]).start()

            @pl.when(jnp.logical_not(own))
            def _():
                pltpu.make_async_copy(blk.at[0, at(js * TILE, TILE), at(k * kc, kc)], stm.at[k], l_stm.at[k]).start()

        def res_copy(c, part):
            b = lax.rem(c, 2)
            return pltpu.make_async_copy(blk.at[1 + part, at(c * CHUNK, CHUNK)], res.at[b, pl.ds(part * CHUNK, CHUNK)], l_fb.at[part])

        def acc_view(t):
            b = lax.rem(t, 2)
            return acc.at[b, pl.ds(0, 2 * CHUNK), :] if is_left else acc.at[b, :, pl.ds(0, 2 * CHUNK)]

        def store_acc(c, t):
            b, half, js = lax.rem(t, 2), lax.div(t, 4), lax.rem(t, 4)

            def views(q, dst):
                src = acc.at[b, pl.ds(q * CHUNK, CHUNK), :] if is_left else acc.at[b, :, pl.ds(q * CHUNK, CHUNK)]
                return pltpu.make_async_copy(src, piece(dst, c, js), l_acc.at[b * 2 + q])

            if is_left:
                return lambda op: (op(views(0, awy.at[half])), op(views(1, out.at[block_of(half), lc])))

            def both(op):
                @pl.when(half == 0)
                def _():
                    for q in range(2):
                        op(views(q, awy.at[kept(q)]))

                @pl.when(half == 1)
                def _():
                    for q in range(2):
                        op(views(q, out.at[q, lc]))

            return both

        def home(c, b):
            return remote(region(out.at[b, lc], is_left, c), region(prv.at[b, lc], is_left, c),
                          s_y.at[c * 2 + b], r_y.at[c * 2 + b], 1 - y, g)

        def spread(c):
            return remote(region(awy.at[0], is_left, c), region(prv.at[2, 0], is_left, c),
                          s_y.at[2 * n_chunk + c], r_y.at[2 * n_chunk + c], 1 - y, g)

        def away(c):
            return remote(region(awy.at[1], is_left, c), region(out.at[y, lc], is_left, c),
                          s_r.at[c], r_r.at[c], y, partner)

        def arrived(c):
            return remote(region(awy.at[1], not is_left, c), region(out.at[y, 1 - lc], not is_left, c),
                          s_r.at[c], r_r.at[c], y, partner)

        def gather(c, owner):
            here = region(out.at[owner, 1 - lc], not is_left, c)
            return remote(here, here, s_y.at[3 * n_chunk + c], r_y.at[3 * n_chunk + c], 1 - y, g)

        def add(c, local, received):
            def view(ref, q):
                return ref.at[0, pl.ds(q * CHUNK, CHUNK), :] if is_left else ref.at[0, :, pl.ds(q * CHUNK, CHUNK)]

            pairs = [(pltpu.make_async_copy(piece(local, c, q), view(fa, q), l_fa.at[q]),
                      pltpu.make_async_copy(piece(received, c, q), view(fb, q), l_fb.at[q])) for q in range(4)]
            for pair in pairs:
                for copy in pair:
                    copy.start()
            stores = [pltpu.make_async_copy(view(fa, q), piece(local, c, q), l_st.at[q]) for q in range(4)]
            for q in range(4):
                for copy in pairs[q]:
                    copy.wait()
                view(fa, q)[...] = view(fa, q)[...] + view(fb, q)[...]
                stores[q].start()
            for q in range(4):
                stores[q].wait()

        def finish_away(c):
            spread(c).wait_recv()
            add(c, awy.at[1], prv.at[2, 0])
            away(c).start()

        def finish_home(c):
            for b in range(2):
                home(c, b).wait_send()
                home(c, b).wait_recv()
                add(c, out.at[b, lc], prv.at[b, lc])

        def forward(c):
            arrived(c).wait_recv()
            gather(c, y).start()

        for k in range(KSTEPS):
            load_stm(0, k)

        def compute(c):
            for part in range(2):
                remote(a.at[0, pl.ds(0, CHUNK)], blk.at[1 + part, at(c * CHUNK, CHUNK)], s_x.at[0], r_x.at[part, c], y, partner).wait_recv()
                res_copy(c, part).start()
            for part in range(2):
                res_copy(c, part).wait()

            def send_half(half):
                if is_left:
                    @pl.when(half == 0)
                    def _():
                        spread(c).start()

                    home(c, block_of(half)).start()
                else:
                    @pl.when(half == 0)
                    def _():
                        spread(c).start()

                    @pl.when(half == 1)
                    def _():
                        for b in range(2):
                            home(c, b).start()

            def tile(t, carry):
                last = lax.div(t + 1, 8)

                def after(k):
                    @pl.when(c + last < n_chunk)
                    def _():
                        load_stm((t + 1) * (1 - last), k)

                    @pl.when(jnp.logical_and(k == 0, t >= 1))
                    def _():
                        store_acc(c, t - 1)(lambda copy: copy.wait())

                        @pl.when(t == 4)
                        def _():
                            send_half(0 * t)

                body_steps(res.at[lax.rem(c, 2), pl.ds(0, 2 * CHUNK), :], acc_view(t), not is_left, after)
                store_acc(c, t)(lambda copy: copy.start())
                return carry

            lax.fori_loop(0, 8, tile, 0)
            store_acc(c, 7)(lambda copy: copy.wait())
            send_half(1 + 0 * c)

        def chunk(c, carry):
            compute(c)

            @pl.when(c >= 1)
            def _():
                finish_away(c - 1)
                finish_home(c - 1)

            return carry

        def forwards(first, stop):
            lax.fori_loop(first, stop, lambda c, carry: (forward(c), carry)[1], 0)

        lax.fori_loop(0, n_chunk, chunk, 0)
        end = n_chunk - 1
        forwards(0, n_chunk // 4)
        finish_away(end)
        forwards(n_chunk // 4, 5 * n_chunk // 8)
        finish_home(end)
        forwards(5 * n_chunk // 8, n_chunk)

        def drain(c, carry):
            spread(c).wait_send()
            away(c).wait_send()
            gather(c, y).wait_send()
            gather(c, 1 - y).wait_recv()
            return carry

        lax.fori_loop(0, n_chunk, drain, 0)
        for layer in range(layers):
            remote(a.at[layer], blk.at[layer], s_d.at[layer], r_d.at[layer], y, mate).wait_send()
        lax.fori_loop(0, n_chunk, x_wait_send, 0)

    pl.when(lax.rem(g, 3) == 0)(diagonal)
    pl.when(g == 1)(lambda: cross(True))
    pl.when(g == 2)(lambda: cross(False))


def solution(mesh):
    assert dict(mesh.shape) == {"m": 1, "kk": 2, "g": 4}
    dma = pltpu.SemaphoreType.DMA

    def local_part(a_loc):
        layers, rows, cols = a_loc.shape
        n_chunk = rows // CHUNK
        any_space = pl.BlockSpec(memory_space=pl.ANY)
        result = pl.pallas_call(
            kernel,
            out_shape=(
                jax.ShapeDtypeStruct((3, layers, rows, rows), F32),
                jax.ShapeDtypeStruct((3, rows, cols), a_loc.dtype),
                jax.ShapeDtypeStruct((3, layers, rows, rows), F32),
                jax.ShapeDtypeStruct((2, rows, rows), F32),
            ),
            in_specs=[any_space],
            out_specs=(any_space,) * 4,
            scratch_shapes=[
                pltpu.VMEM((2, TILE, cols), a_loc.dtype),
                pltpu.VMEM((KSTEPS, TILE, cols // KSTEPS), a_loc.dtype),
                pltpu.VMEM((2, TILE, TILE), F32),
                pltpu.VMEM((2, TILE, TILE), F32),
                pltpu.VMEM((2, TILE, TILE), F32),
                pltpu.VMEM((2, TILE, TILE), F32),
                dma((n_chunk,)), dma((2, n_chunk)), dma((2,)), dma((2,)),
                dma((4 * n_chunk,)), dma((4 * STRIPS,)), dma((n_chunk,)), dma((n_chunk,)),
                dma((2,)), dma((KSTEPS,)), dma((4,)), dma((4,)), dma((4,)), dma((4,)), dma((2,)),
            ],
            compiler_params=pltpu.CompilerParams(
                collective_id=0, has_side_effects=True, vmem_limit_bytes=63 * 2**20),
            cost_estimate=pl.CostEstimate(flops=10**12, bytes_accessed=10**9, transcendentals=0),
        )(a_loc)
        return result[0][None]

    return jax.shard_map(local_part, mesh=mesh, in_specs=(P(None, ("m", "g"), "kk"),),
                         out_specs=P(("m", "g"), None, None, None, None), check_vma=False)
```

```python
import jax
import jax.numpy as jnp
from jax import lax
from jax.experimental import pallas as pl
from jax.experimental.pallas import tpu as pltpu
from jax.sharding import PartitionSpec as P


MESH = pl.DeviceIdType.MESH
NT = (((1,), (1,)), ((), ()))
F32 = jnp.float32

TILE = 512
CHUNK = 128
STRIPS = 24
KSTEPS = 2
LAG = 4
INSIDE = 5
PIECES = ((5, 6), (6, 7), (7, 9), (9, 11), (11, 13), (13, 15), (15, 16))


def kernel(a, out, blk, prv, awy, late, *refs):
    pieces, refs = refs[:len(PIECES)], refs[len(PIECES):]
    work(a, out, blk, prv, awy, late, pieces, *refs)


def work(a, out, blk, prv, awy, late, pieces, res, stm, acc, fa, fb, fc,
           s_x, r_x, s_d, r_d, s_y, r_y, s_r, r_r,
           l_res, l_stm, l_acc, l_fa, l_fb, l_st, l_tr):
    m = lax.axis_index("m")
    y = lax.axis_index("kk")
    g = lax.axis_index("g")
    side = lax.div(g, 2)
    layers, rows, cols = a.shape
    kc = cols // KSTEPS
    n_strip = rows // TILE
    n_chunk = rows // CHUNK

    def at(start, size):
        return pl.ds(pl.multiple_of(start, size), size)

    def remote(src, dst, ss, rs, kk2, g2):
        return pltpu.make_async_remote_copy(src, dst, ss, rs, device_id=(m, kk2, g2), device_id_type=MESH)

    barrier = pltpu.get_barrier_semaphore()
    me = y * 4 + g
    for step in range(1, 8):
        other = lax.rem(me + step, 8)
        pl.semaphore_signal(barrier, inc=1, device_id=(m, lax.div(other, 4), lax.rem(other, 4)), device_id_type=MESH)
    pl.semaphore_wait(barrier, 7)

    def x_in(c):
        part = lax.rem(g, 2)
        return remote(a.at[1 - side, at(c * CHUNK, CHUNK)], blk.at[1 + part, at(c * CHUNK, CHUNK)],
                      s_x.at[c], r_x.at[part, c], y, 2 - side)

    def x_start(c, carry):
        x_in(c).start()
        return carry

    def x_wait_send(c, carry):
        x_in(c).wait_send()
        return carry

    def body_steps(res_view, acc_view, swap, before, after):
        acc_view[...] = jnp.zeros(acc_view.shape, F32)

        def step(k, carry):
            before(k)
            pltpu.make_async_copy(a.at[0, pl.ds(0, TILE), pl.ds(0, kc)], stm.at[k], l_stm.at[k]).wait()
            lhs = res_view[:, at(k * kc, kc)]
            rhs = stm[k]
            if swap:
                lhs, rhs = rhs, lhs
            acc_view[...] += lax.dot_general(lhs, rhs, NT, preferred_element_type=F32)
            after(k)
            return carry

        lax.fori_loop(0, KSTEPS, step, 0)

    def diagonal():
        d = lax.div(g, 3)
        mate = g + 1 - 2 * d
        d2d = remote(a.at[side], blk.at[0], s_d.at[0], r_d.at[0], y, mate)

        def phase(r):
            return lax.div(r, 8), lax.rem(lax.div(r, 4), 2), n_strip - 1 - lax.rem(r, 4)

        def count(r):
            p, _, i = phase(r)
            return (i + 1) + lax.rem(p, 2) * (n_strip - 1 - i)

        def slot(p):
            return p * (1 - 2 * d) + 2 * d

        def load(own, layer, row, col, width, dst, sem):
            @pl.when(own)
            def _():
                pltpu.make_async_copy(a.at[layer, at(row, TILE), at(col, width)], dst, sem).start()

            @pl.when(jnp.logical_not(own))
            def _():
                pltpu.make_async_copy(blk.at[layer, at(row, TILE), at(col, width)], dst, sem).start()

        def load_res(r, k):
            p, layer, i = phase(r)
            own = p + 1 - d < 2
            load(own, layer, i * TILE, k * kc, kc, res.at[lax.rem(r, 2), :, at(k * kc, kc)], l_res.at[lax.rem(r, 2) * KSTEPS + k])

        def load_stm(r, j, k):
            p, layer, _ = phase(r)
            own = p + d < 2
            load(own, layer, j * TILE, k * kc, kc, stm.at[k], l_stm.at[k])

        def tile_of(ref, r, i, j):
            p, layer, _ = phase(r)
            return ref.at[slot(p), layer, at(i * TILE, TILE), at(j * TILE, TILE)]

        def is_diag(r, j):
            p, _, i = phase(r)
            return jnp.logical_and(p != 1, i == j)

        def is_mirror(r, j):
            p, _, i = phase(r)
            return jnp.logical_and(p != 1, i != j)

        def whole(r, j):
            i = phase(r)[2]
            return remote(tile_of(out, r, i, j), tile_of(prv, r, i, j),
                          s_y.at[lax.rem(r, 8) * 4 + j], r_y.at[r * 4 + j], 1 - y, g)

        def lower(r, j, row, height, width):
            p, layer, i = phase(r)

            def part(ref):
                return ref.at[slot(p), layer, pl.ds(pl.multiple_of(i * TILE + row, 128), height), pl.ds(pl.multiple_of(j * TILE, TILE), width)]

            return remote(part(out), part(prv), s_y.at[lax.rem(r, 8) * 4 + j], r_y.at[r * 4 + j], 1 - y, g)

        def send(r, j):
            @pl.when(is_diag(r, j))
            def _():
                for q in range(4):
                    lower(r, j, q * 128, 128, (q + 1) * 128).start()

            @pl.when(jnp.logical_not(is_diag(r, j)))
            def _():
                whole(r, j).start()

        def wait_exchange(r, j):
            @pl.when(is_diag(r, j))
            def _():
                sized = lower(r, j, 0, 320, TILE)
                sized.wait_send()
                sized.wait_recv()

            @pl.when(jnp.logical_not(is_diag(r, j)))
            def _():
                whole(r, j).wait_send()
                whole(r, j).wait_recv()

        def store_acc(r, j):
            return pltpu.make_async_copy(acc.at[lax.rem(j, 2)], tile_of(out, r, phase(r)[2], j), l_acc.at[lax.rem(j, 2)])

        def finish(r):
            n = count(r)
            i = phase(r)[2]

            def loads(j):
                b = lax.rem(j, 2)
                return (pltpu.make_async_copy(tile_of(out, r, i, j), fa.at[b], l_fa.at[b]),
                        pltpu.make_async_copy(tile_of(prv, r, i, j), fb.at[b], l_fb.at[b]))

            def start_loads(j):
                wait_exchange(r, j)
                for copy in loads(j):
                    copy.start()

            def main_store(j):
                return pltpu.make_async_copy(fa.at[lax.rem(j, 2)], tile_of(out, r, i, j), l_st.at[lax.rem(j, 2)])

            def mirror_store(j):
                return pltpu.make_async_copy(fc.at[lax.rem(j, 2)], tile_of(out, r, j, i), l_tr.at[lax.rem(j, 2)])

            def wait_stores(j):
                main_store(j).wait()

                @pl.when(is_mirror(r, j))
                def _():
                    mirror_store(j).wait()

            start_loads(0)

            def one(j, carry):
                b = lax.rem(j, 2)

                @pl.when(j + 1 < n)
                def _():
                    @pl.when(j >= 1)
                    def _():
                        wait_stores(j - 1)

                    start_loads(j + 1)

                for copy in loads(j):
                    copy.wait()
                fa[b] = fa[b] + fb[b]

                @pl.when(is_mirror(r, j))
                def _():
                    fc[b] = fa[b].T
                    mirror_store(j).start()

                @pl.when(is_diag(r, j))
                def _():
                    total = fa[b]
                    at_row = lax.broadcasted_iota(jnp.int32, (TILE, TILE), 0)
                    at_col = lax.broadcasted_iota(jnp.int32, (TILE, TILE), 1)
                    fa[b] = jnp.where(at_row >= at_col, total, total.T)

                main_store(j).start()
                return carry

            lax.fori_loop(0, n, one, 0)

            @pl.when(n >= 2)
            def _():
                wait_stores(n - 2)

            wait_stores(n - 1)

        for k in range(KSTEPS):
            load_res(0, k)
            load_stm(0, 0, k)
        d2d.start()
        lax.fori_loop(0, n_chunk, x_start, 0)

        def strip(r, carry):
            @pl.when(r == 7)
            def _():
                remote(a.at[0], blk.at[0], s_d.at[0], r_d.at[0], y, mate).wait_recv()

            @pl.when(r == 11)
            def _():
                remote(a.at[1], blk.at[1], s_d.at[1], r_d.at[1], y, mate).wait_recv()

            @pl.when(jnp.logical_and(r >= 1, r + 1 < STRIPS))
            def _():
                for k in range(KSTEPS):
                    load_res(r + 1, k)

            n = count(r)

            def tile(j, carry):
                last = lax.div(j + 1, n)

                def before(k):
                    @pl.when(j == 0)
                    def _():
                        b = lax.rem(r, 2)
                        pltpu.make_async_copy(a.at[0, pl.ds(0, TILE), pl.ds(0, kc)], res.at[b, :, pl.ds(0, kc)], l_res.at[b * KSTEPS + k]).wait()

                def after(k):
                    @pl.when(jnp.logical_and(r == 0, j == 0))
                    def _():
                        load_res(r + 1, k)

                    @pl.when(r + last < STRIPS)
                    def _():
                        load_stm(r + last, (j + 1) * (1 - last), k)

                    @pl.when(jnp.logical_and(k == 0, j >= 1))
                    def _():
                        store_acc(r, j - 1).wait()
                        send(r, j - 1)

                body_steps(res.at[lax.rem(r, 2)], acc.at[lax.rem(j, 2)], False, before, after)
                store_acc(r, j).start()
                return carry

            lax.fori_loop(0, n, tile, 0)
            store_acc(r, n - 1).wait()
            send(r, n - 1)

            @pl.when(r >= LAG)
            def _():
                finish(r - LAG)

            return carry

        lax.fori_loop(0, STRIPS, strip, 0)
        lax.fori_loop(STRIPS - LAG, STRIPS, lambda r, carry: (finish(r), carry)[1], 0)
        d2d.wait_send()
        lax.fori_loop(0, n_chunk, x_wait_send, 0)

    def cross(is_left):
        lc = 0 if is_left else 1
        mate = 0 if is_left else 3
        partner = 2 if is_left else 1
        for layer in range(layers):
            remote(a.at[layer], blk.at[layer], s_d.at[layer], r_d.at[layer], y, mate).start()
        lax.fori_loop(0, n_chunk, x_start, 0)

        remote(a.at[lc], blk.at[0], s_d.at[0], r_d.at[0], y, mate).wait_recv()

        def region(ref, rows_first, c):
            return ref.at[at(c * CHUNK, CHUNK), :] if rows_first else ref.at[:, at(c * CHUNK, CHUNK)]

        def piece(ref, c, q):
            if is_left:
                return ref.at[at(c * CHUNK, CHUNK), at(q * TILE, TILE)]
            return ref.at[at(q * TILE, TILE), at(c * CHUNK, CHUNK)]

        def block_of(half):
            return lax.rem(half + 1 - y + 2, 2)

        def kept(b):
            return lax.rem(b + 1 - y + 2, 2)

        def load_stm(t, k):
            half, js = lax.div(t, 4), lax.rem(t, 4)
            own = block_of(half) == 1 if is_left else half == 1

            @pl.when(own)
            def _():
                pltpu.make_async_copy(a.at[lc, at(js * TILE, TILE), at(k * kc, kc)], stm.at[k], l_stm.at[k]).start()

            @pl.when(jnp.logical_not(own))
            def _():
                pltpu.make_async_copy(blk.at[0, at(js * TILE, TILE), at(k * kc, kc)], stm.at[k], l_stm.at[k]).start()

        def res_copy(c, part):
            b = lax.rem(c, 2)
            return pltpu.make_async_copy(blk.at[1 + part, at(c * CHUNK, CHUNK)], res.at[b, pl.ds(part * CHUNK, CHUNK)], l_fb.at[part])

        def acc_view(t):
            b = lax.rem(t, 2)
            return acc.at[b, pl.ds(0, 2 * CHUNK), :] if is_left else acc.at[b, :, pl.ds(0, 2 * CHUNK)]

        def store_acc(c, t):
            b, half, js = lax.rem(t, 2), lax.div(t, 4), lax.rem(t, 4)

            def views(q, dst):
                src = acc.at[b, pl.ds(q * CHUNK, CHUNK), :] if is_left else acc.at[b, :, pl.ds(q * CHUNK, CHUNK)]
                return pltpu.make_async_copy(src, piece(dst, c, js), l_acc.at[b * 2 + q])

            if is_left:
                return lambda op: (op(views(0, awy.at[half])), op(views(1, out.at[block_of(half), lc])))

            def both(op):
                @pl.when(half == 0)
                def _():
                    for q in range(2):
                        op(views(q, awy.at[kept(q)]))

                @pl.when(half == 1)
                def _():
                    for q in range(2):
                        op(views(q, out.at[q, lc]))

            return both

        def home(c, b):
            return remote(region(out.at[b, lc], is_left, c), region(prv.at[b, lc], is_left, c),
                          s_y.at[c * 2 + b], r_y.at[c * 2 + b], 1 - y, g)

        def spread(c):
            return remote(region(awy.at[0], is_left, c), region(prv.at[2, 0], is_left, c),
                          s_y.at[2 * n_chunk + c], r_y.at[2 * n_chunk + c], 1 - y, g)

        def away(c):
            return remote(region(awy.at[1], is_left, c), region(out.at[y, lc], is_left, c),
                          s_r.at[c], r_r.at[c], y, partner)

        def arrived(c):
            return remote(region(awy.at[1], not is_left, c), region(out.at[y, 1 - lc], not is_left, c),
                          s_r.at[c], r_r.at[c], y, partner)

        def away_late():
            return remote(pieces[0], late, s_r.at[INSIDE], r_r.at[INSIDE], y, partner)

        def gather(c, owner):
            here = region(out.at[owner, 1 - lc], not is_left, c)
            return remote(here, here, s_y.at[3 * n_chunk + c], r_y.at[3 * n_chunk + c], 1 - y, g)

        def add(c, local, received, store=None):
            def view(ref, q):
                return ref.at[0, pl.ds(q * CHUNK, CHUNK), :] if is_left else ref.at[0, :, pl.ds(q * CHUNK, CHUNK)]

            pairs = [(pltpu.make_async_copy(piece(local, c, q), view(fa, q), l_fa.at[q]),
                      pltpu.make_async_copy(piece(received, c, q), view(fb, q), l_fb.at[q])) for q in range(4)]
            for pair in pairs:
                for copy in pair:
                    copy.start()
            stores = [pltpu.make_async_copy(view(fa, q), piece(local, c, q), l_st.at[q]) for q in range(4)]
            for q in range(4):
                for copy in pairs[q]:
                    copy.wait()
                view(fa, q)[...] = view(fa, q)[...] + view(fb, q)[...]
                if store is None:
                    stores[q].start()
                else:
                    store(q, view(fa, q), stores[q])
            for q in range(4):
                stores[q].wait()

        def finish_away(c):
            spread(c).wait_recv()

            def store(q, total, inside):
                @pl.when(c < INSIDE)
                def _():
                    inside.start()

                for (first, stop), piece_ref in zip(PIECES, pieces):
                    @pl.when(jnp.logical_and(c >= first, c < stop))
                    def _(first=first, piece_ref=piece_ref):
                        if is_left:
                            pltpu.make_async_copy(total, piece_ref.at[c - first, :, pl.ds(q * TILE, TILE)], l_st.at[q]).start()
                        else:
                            for u in range(TILE // CHUNK):
                                pltpu.make_async_copy(total.at[pl.ds(u * CHUNK, CHUNK), :],
                                                      piece_ref.at[c - first, :, pl.ds(q * TILE + u * CHUNK, CHUNK)], l_st.at[q]).start()

            add(c, awy.at[1], prv.at[2, 0], store)

            @pl.when(c < INSIDE)
            def _():
                away(c).start()

            @pl.when(c == INSIDE)
            def _():
                away_late().start()

        def finish_home(c):
            for b in range(2):
                home(c, b).wait_send()
                home(c, b).wait_recv()
                add(c, out.at[b, lc], prv.at[b, lc])

        def forward(c):
            arrived(c).wait_recv()
            gather(c, y).start()

        for k in range(KSTEPS):
            load_stm(0, k)

        def compute(c):
            for part in range(2):
                remote(a.at[0, pl.ds(0, CHUNK)], blk.at[1 + part, at(c * CHUNK, CHUNK)], s_x.at[0], r_x.at[part, c], y, partner).wait_recv()
                res_copy(c, part).start()
            for part in range(2):
                res_copy(c, part).wait()

            def send_half(half):
                if is_left:
                    @pl.when(half == 0)
                    def _():
                        spread(c).start()

                    home(c, block_of(half)).start()
                else:
                    @pl.when(half == 0)
                    def _():
                        spread(c).start()

                    @pl.when(half == 1)
                    def _():
                        for b in range(2):
                            home(c, b).start()

            def tile(t, carry):
                last = lax.div(t + 1, 8)

                def after(k):
                    @pl.when(c + last < n_chunk)
                    def _():
                        load_stm((t + 1) * (1 - last), k)

                    @pl.when(jnp.logical_and(k == 0, t >= 1))
                    def _():
                        store_acc(c, t - 1)(lambda copy: copy.wait())

                        @pl.when(t == 4)
                        def _():
                            send_half(0 * t)

                        @pl.when(jnp.logical_and(c == n_chunk - 1, lax.rem(t, 2) == 1))
                        def _():
                            forward(lax.div(t, 2))

                body_steps(res.at[lax.rem(c, 2), pl.ds(0, 2 * CHUNK), :], acc_view(t), not is_left, lambda k: None, after)
                store_acc(c, t)(lambda copy: copy.start())
                return carry

            lax.fori_loop(0, 8, tile, 0)
            store_acc(c, 7)(lambda copy: copy.wait())
            send_half(1 + 0 * c)

        def chunk(c, carry):
            compute(c)

            @pl.when(c >= 1)
            def _():
                finish_away(c - 1)
                finish_home(c - 1)

            return carry

        lax.fori_loop(0, n_chunk, chunk, 0)
        for c in range(4, INSIDE):
            forward(c)
        finish_away(n_chunk - 1)
        finish_home(n_chunk - 1)

        def drain(c, carry):
            away(c).wait_send()
            gather(c, y).wait_send()
            gather(c, 1 - y).wait_recv()
            return carry

        def drain_spread(c, carry):
            spread(c).wait_send()
            return carry

        lax.fori_loop(0, INSIDE, drain, 0)
        lax.fori_loop(0, n_chunk, drain_spread, 0)
        away_late().wait_send()
        away_late().wait_recv()
        for layer in range(layers):
            remote(a.at[layer], blk.at[layer], s_d.at[layer], r_d.at[layer], y, mate).wait_send()
        lax.fori_loop(0, n_chunk, x_wait_send, 0)

    pl.when(lax.rem(g, 3) == 0)(diagonal)
    pl.when(g == 1)(lambda: cross(True))
    pl.when(g == 2)(lambda: cross(False))


def assembly(step, first, *refs):
    n_in = len(first) + (step <= 2)
    ins, (out, *scratch) = refs[:n_in], refs[n_in:]
    buf, wide, l_in, l_out, l_win, l_wout = scratch
    y = lax.axis_index("kk")
    g = lax.axis_index("g")
    depth = buf.shape[0]
    lead = depth // 2

    def at(start, size):
        return pl.ds(pl.multiple_of(start, size), size)

    def copies(n, where):
        src = ins[-1]

        def view(ref, t):
            slot, layer, i, j = where(t)
            return ref.at[slot, layer, at(i * TILE, TILE), at(j * TILE, TILE)]

        def load(t):
            b = lax.rem(t, depth)
            return pltpu.make_async_copy(view(src, t), buf.at[b], l_in.at[b])

        def store(t):
            b = lax.rem(t, depth)
            return pltpu.make_async_copy(buf.at[b], view(out, t), l_out.at[b])

        def one(t, carry):
            @pl.when(jnp.logical_and(t >= depth, t < n))
            def _():
                store(t - depth).wait()

            @pl.when(t < n)
            def _():
                load(t).start()

            @pl.when(t >= lead)
            def _():
                load(t - lead).wait()
                store(t - lead).start()

            return carry

        lax.fori_loop(0, n + lead, one, 0)

        def last(t, carry):
            store(t).wait()
            return carry

        lax.fori_loop(max(n - depth, 0), n, last, 0)

    def zeros():
        buf[0] = jnp.zeros((TILE, TILE), F32)

        def store(b, layer, t):
            return pltpu.make_async_copy(buf.at[0], out.at[2, layer, at(lax.div(t, 4) * TILE, TILE), at(lax.rem(t, 4) * TILE, TILE)], l_out.at[b])

        for layer in range(2):
            for t in range(16):
                store(t, layer, t).start()
            for t in range(16):
                store(t, layer, t).wait()

    def away_results(is_left):
        layer = 1 if is_left else 0
        todo = [(k, c, n, (y if ours else 1 - y)) for k, (lo, hi, ours) in enumerate(first) for n, c in enumerate(range(lo, hi))]

        def load(t):
            k, _, n, _ = todo[t]
            return pltpu.make_async_copy(ins[k].at[n], wide.at[t], l_win.at[t])

        def whole(t):
            _, c, _, slot = todo[t]
            return pltpu.make_async_copy(wide.at[t], out.at[slot, layer, pl.ds(c * CHUNK, CHUNK), :], l_wout.at[t])

        for t in range(len(todo)):
            load(t).start()
        for t in range(len(todo)):
            _, c, _, slot = todo[t]
            load(t).wait()
            if not is_left:
                whole(t).start()
            else:
                for u in range(out.shape[2] // CHUNK):
                    pltpu.make_async_copy(wide.at[t, :, pl.ds(u * CHUNK, CHUNK)],
                                          out.at[slot, layer, pl.ds(u * CHUNK, CHUNK), pl.ds(c * CHUNK, CHUNK)], l_wout.at[t]).start()
        for t in range(len(todo)):
            whole(t).wait()

    def on_cross(is_left):
        lc = 0 if is_left else 1
        away_results(is_left)
        if step == 0:
            if is_left:
                copies(16, lambda t: (lax.div(t, 8), 1 - lc, lax.rem(lax.div(t, 2), 4), lax.rem(t, 2)))
            else:
                copies(16, lambda t: (lax.div(t, 8), 1 - lc, lax.rem(lax.div(t, 4), 2), lax.rem(t, 4)))
        elif step <= 2:
            copies(16, lambda t: (step - 1, lc, lax.div(t, 4), lax.rem(t, 4)))
        elif step == 3:
            zeros()

    @pl.when(g == 1)
    def _():
        on_cross(True)

    @pl.when(g == 2)
    def _():
        on_cross(False)

    if step < 3:
        @pl.when(lax.rem(g, 3) == 0)
        def _():
            copies(32, lambda t: (step, lax.div(t, 16), lax.div(lax.rem(t, 16), 4), lax.rem(t, 4)))


def solution(mesh):
    assert dict(mesh.shape) == {"m": 1, "kk": 2, "g": 4}
    dma = pltpu.SemaphoreType.DMA

    def local_part(a_loc):
        layers, rows, cols = a_loc.shape
        n_chunk = rows // CHUNK
        any_space = pl.BlockSpec(memory_space=pl.ANY)
        slots_shape = jax.ShapeDtypeStruct((3, layers, rows, rows), F32)

        def chunks_shape(n):
            return jax.ShapeDtypeStruct((n, CHUNK, rows), F32)

        slots, _, _, _, late, *pieces = pl.pallas_call(
            kernel,
            out_shape=(
                slots_shape,
                jax.ShapeDtypeStruct((3, rows, cols), a_loc.dtype),
                slots_shape,
                jax.ShapeDtypeStruct((2, rows, rows), F32),
                chunks_shape(1),
                *(chunks_shape(stop - start) for start, stop in PIECES),
            ),
            in_specs=[any_space],
            out_specs=(any_space,) * (5 + len(PIECES)),
            scratch_shapes=[
                pltpu.VMEM((2, TILE, cols), a_loc.dtype),
                pltpu.VMEM((KSTEPS, TILE, cols // KSTEPS), a_loc.dtype),
                pltpu.VMEM((2, TILE, TILE), F32),
                pltpu.VMEM((2, TILE, TILE), F32),
                pltpu.VMEM((2, TILE, TILE), F32),
                pltpu.VMEM((2, TILE, TILE), F32),
                dma((n_chunk,)), dma((2, n_chunk)), dma((2,)), dma((2,)),
                dma((4 * n_chunk,)), dma((4 * STRIPS,)), dma((n_chunk,)), dma((n_chunk,)),
                dma((2 * KSTEPS,)), dma((KSTEPS,)), dma((4,)), dma((4,)), dma((4,)), dma((4,)), dma((2,)),
            ],
            compiler_params=pltpu.CompilerParams(
                collective_id=0, has_side_effects=True, vmem_limit_bytes=63 * 2**20),
            cost_estimate=pl.CostEstimate(flops=10**12, bytes_accessed=10**9, transcendentals=0),
        )(a_loc)

        other_chip = [(1, 2), (2, 1)]
        other_half = [(1, 5), (5, 1), (2, 6), (6, 2)]

        mine = [late] + [lax.ppermute(pieces[k], "g", other_chip) for k in range(1, len(PIECES))]
        theirs = [lax.ppermute(mine[k], ("kk", "g"), other_half) for k in range(len(PIECES))]

        def assemble(step, result, parts):
            first = tuple(PIECES[k] + (ours,) for k, ours in parts)
            arrays = [mine[k] if ours else theirs[k] for k, ours in parts]
            n_wide = max(1, sum(stop - start for start, stop, _ in first))
            sources = arrays + ([slots] if step <= 2 else [])
            aliases = {}
            operands = sources
            if step > 0:
                operands = [result] + sources
                aliases = {0: 0}

            def body(*refs):
                assembly(step, first, *refs[len(operands) - len(sources):])

            return pl.pallas_call(
                body,
                out_shape=slots_shape,
                in_specs=[any_space] * len(operands),
                out_specs=any_space,
                input_output_aliases=aliases,
                scratch_shapes=[
                    pltpu.VMEM((16, TILE, TILE), F32), pltpu.VMEM((n_wide, CHUNK, rows), F32),
                    dma((16,)), dma((16,)), dma((n_wide,)), dma((n_wide,)),
                ],
                compiler_params=pltpu.CompilerParams(vmem_limit_bytes=67043328),
                cost_estimate=pl.CostEstimate(flops=10**10, bytes_accessed=10**8, transcendentals=0),
            )(*operands)

        result = assemble(0, None, [])
        result = assemble(1, result, [(1, True)])
        result = assemble(2, result, [(2, True), (0, True), (0, False)])
        result = assemble(3, result, [(3, True), (1, False)])
        result = assemble(4, result, [(4, True), (2, False)])
        result = assemble(5, result, [(5, True), (3, False)])
        result = assemble(6, result, [(6, True), (4, False)])
        result = assemble(7, result, [(5, False), (6, False)])
        return result[None]

    return jax.shard_map(local_part, mesh=mesh, in_specs=(P(None, ("m", "g"), "kk"),),
                         out_specs=P(("m", "g"), None, None, None, None), check_vma=False)
```

```python
import jax
import jax.numpy as jnp
from jax import lax
from jax.experimental import pallas as pl
from jax.experimental.pallas import tpu as pltpu
from jax.sharding import PartitionSpec as P


MESH = pl.DeviceIdType.MESH
NT = (((1,), (1,)), ((), ()))
F32 = jnp.float32

TILE = 512
CHUNK = 128
STRIPS = 24
KSTEPS = 2
LAG = 4
PACKED = 264
WHOLE = 2
INSIDE = 4
PIECES = ((4, 8), (8, 11), (11, 14), (14, 16))


def kernel(a, out, blk, prv, awy, pkl, pkr, late, *refs):
    both, pieces, refs = refs[:WHOLE], refs[WHOLE:WHOLE + len(PIECES)], refs[WHOLE + len(PIECES):]
    work(a, out, blk, prv, awy, pkl, pkr, late, both, pieces, *refs)


def work(a, out, blk, prv, awy, pkl, pkr, late, both, pieces, res, stm, acc, fa, fb, fc, pk, fpa, fpb,
         s_x, r_x, s_d, r_d, s_y, r_y, s_r, r_r,
         l_res, l_stm, l_acc, l_fa, l_fb, l_st, l_tr, l_pk):
    m = lax.axis_index("m")
    y = lax.axis_index("kk")
    g = lax.axis_index("g")
    side = lax.div(g, 2)
    layers, rows, cols = a.shape
    kc = cols // KSTEPS
    n_strip = rows // TILE
    n_chunk = rows // CHUNK

    def at(start, size):
        return pl.ds(pl.multiple_of(start, size), size)

    def remote(src, dst, ss, rs, kk2, g2):
        return pltpu.make_async_remote_copy(src, dst, ss, rs, device_id=(m, kk2, g2), device_id_type=MESH)

    def enter():
        barrier = pltpu.get_barrier_semaphore()
        me = y * 4 + g
        for step in range(1, 8):
            other = lax.rem(me + step, 8)
            pl.semaphore_signal(barrier, inc=1, device_id=(m, lax.div(other, 4), lax.rem(other, 4)), device_id_type=MESH)
        pl.semaphore_wait(barrier, 7)

    def x_in(c):
        part = lax.rem(g, 2)
        return remote(a.at[1 - side, at(c * CHUNK, CHUNK)], blk.at[1 + part, at(c * CHUNK, CHUNK)],
                      s_x.at[c], r_x.at[part, c], y, 2 - side)

    def x_start(c, carry):
        x_in(c).start()
        return carry

    def x_wait_send(c, carry):
        x_in(c).wait_send()
        return carry

    def body_steps(res_view, acc_view, swap, before, after):
        acc_view[...] = jnp.zeros(acc_view.shape, F32)

        def step(k, carry):
            before(k)
            pltpu.make_async_copy(a.at[0, pl.ds(0, TILE), pl.ds(0, kc)], stm.at[k], l_stm.at[k]).wait()
            lhs = res_view[:, at(k * kc, kc)]
            rhs = stm[k]
            if swap:
                lhs, rhs = rhs, lhs
            acc_view[...] += lax.dot_general(lhs, rhs, NT, preferred_element_type=F32)
            after(k)
            return carry

        lax.fori_loop(0, KSTEPS, step, 0)

    def diagonal():
        d = lax.div(g, 3)
        mate = g + 1 - 2 * d
        d2d = remote(a.at[side], blk.at[0], s_d.at[0], r_d.at[0], y, mate)

        def phase(r):
            return lax.div(r, 8), lax.rem(lax.div(r, 4), 2), n_strip - 1 - lax.rem(r, 4)

        def count(r):
            p, _, i = phase(r)
            return (i + 1) + lax.rem(p, 2) * (n_strip - 1 - i)

        def slot(p):
            return p * (1 - 2 * d) + 2 * d

        def load(own, layer, row, col, width, dst, sem):
            @pl.when(own)
            def _():
                pltpu.make_async_copy(a.at[layer, at(row, TILE), at(col, width)], dst, sem).start()

            @pl.when(jnp.logical_not(own))
            def _():
                pltpu.make_async_copy(blk.at[layer, at(row, TILE), at(col, width)], dst, sem).start()

        def load_res(r, k):
            p, layer, i = phase(r)
            own = p + 1 - d < 2
            load(own, layer, i * TILE, k * kc, kc, res.at[lax.rem(r, 2), :, at(k * kc, kc)], l_res.at[lax.rem(r, 2) * KSTEPS + k])

        def load_stm(r, j, k):
            p, layer, _ = phase(r)
            own = p + d < 2
            load(own, layer, j * TILE, k * kc, kc, stm.at[k], l_stm.at[k])

        def tile_of(ref, r, i, j):
            p, layer, _ = phase(r)
            return ref.at[slot(p), layer, at(i * TILE, TILE), at(j * TILE, TILE)]

        def is_diag(r, j):
            p, _, i = phase(r)
            return jnp.logical_and(p != 1, i == j)

        def is_mirror(r, j):
            p, _, i = phase(r)
            return jnp.logical_and(p != 1, i != j)

        def whole(r, j):
            i = phase(r)[2]
            return remote(tile_of(out, r, i, j), tile_of(prv, r, i, j),
                          s_y.at[lax.rem(r, 8) * 4 + j], r_y.at[r * 4 + j], 1 - y, g)

        def lower(r, j, row, height, width):
            p, layer, i = phase(r)

            def part(ref):
                return ref.at[slot(p), layer, pl.ds(pl.multiple_of(i * TILE + row, 128), height), pl.ds(pl.multiple_of(j * TILE, TILE), width)]

            return remote(part(out), part(prv), s_y.at[lax.rem(r, 8) * 4 + j], r_y.at[r * 4 + j], 1 - y, g)

        def packed(r):
            e = lax.rem(r, 8) + 8 * lax.div(phase(r)[0], 2)
            return remote(pkl.at[e], pkr.at[e], s_y.at[32 + lax.rem(r, 8)], r_y.at[4 * STRIPS + e], 1 - y, g)

        def store_packed(r):
            return pltpu.make_async_copy(pk, pkl.at[lax.rem(r, 8) + 8 * lax.div(phase(r)[0], 2)], l_pk.at[0])

        def load_packed(r):
            e = lax.rem(r, 8) + 8 * lax.div(phase(r)[0], 2)
            return pltpu.make_async_copy(pkl.at[e], fpa, l_pk.at[1]), pltpu.make_async_copy(pkr.at[e], fpb, l_pk.at[2])

        row_id = lax.broadcasted_iota(jnp.int32, (128, 128), 0)
        col_id = lax.broadcasted_iota(jnp.int32, (128, 128), 1)

        def pack(tile):
            ends = []
            for h in range(2):
                one, two = 256 * h, 256 * h + 128
                first = tile[pl.ds(one, 128), pl.ds(one, 128)]
                second = tile[pl.ds(two, 128), pl.ds(two, 128)]
                pk[pl.ds(128 * h, 128), :] = jnp.where(row_id > col_id, first, second.T)
                ends.append(jnp.sum(jnp.where(row_id == col_id, first, 0.0), axis=0, keepdims=True))
            pk[pl.ds(256, 8), :] = jnp.where(row_id[:8] == 0, ends[0], ends[1])

        def unpack(tile):
            fpa[...] = fpa[...] + fpb[...]
            for h in range(2):
                one, two = 256 * h, 256 * h + 128
                both = fpa[pl.ds(128 * h, 128), :]
                turned = both.T
                ends = fpa[pl.ds(256 + h, 1), :]
                tile[pl.ds(one, 128), pl.ds(one, 128)] = jnp.where(row_id > col_id, both, jnp.where(row_id == col_id, ends, turned))
                tile[pl.ds(two, 128), pl.ds(two, 128)] = jnp.where(row_id <= col_id, both, turned)

        def send(r, j):
            @pl.when(is_diag(r, j))
            def _():
                for q in range(1, 4):
                    lower(r, j, q * 128, 128, q * 128).start()
                store_packed(r).wait()
                packed(r).start()

            @pl.when(jnp.logical_not(is_diag(r, j)))
            def _():
                whole(r, j).start()

        def wait_exchange(r, j):
            @pl.when(is_diag(r, j))
            def _():
                sized = lower(r, j, 0, 192, TILE)
                sized.wait_send()
                sized.wait_recv()
                packed(r).wait_send()
                packed(r).wait_recv()

            @pl.when(jnp.logical_not(is_diag(r, j)))
            def _():
                whole(r, j).wait_send()
                whole(r, j).wait_recv()

        def store_acc(r, j):
            return pltpu.make_async_copy(acc.at[lax.rem(j, 2)], tile_of(out, r, phase(r)[2], j), l_acc.at[lax.rem(j, 2)])

        def finish(r):
            n = count(r)
            i = phase(r)[2]

            def loads(j):
                b = lax.rem(j, 2)
                return (pltpu.make_async_copy(tile_of(out, r, i, j), fa.at[b], l_fa.at[b]),
                        pltpu.make_async_copy(tile_of(prv, r, i, j), fb.at[b], l_fb.at[b]))

            def start_loads(j):
                wait_exchange(r, j)
                for copy in loads(j):
                    copy.start()

                @pl.when(is_diag(r, j))
                def _():
                    for copy in load_packed(r):
                        copy.start()

            def main_store(j):
                return pltpu.make_async_copy(fa.at[lax.rem(j, 2)], tile_of(out, r, i, j), l_st.at[lax.rem(j, 2)])

            def mirror_store(j):
                return pltpu.make_async_copy(fc.at[lax.rem(j, 2)], tile_of(out, r, j, i), l_tr.at[lax.rem(j, 2)])

            def wait_stores(j):
                main_store(j).wait()

                @pl.when(is_mirror(r, j))
                def _():
                    mirror_store(j).wait()

            start_loads(0)

            def one(j, carry):
                b = lax.rem(j, 2)

                @pl.when(j + 1 < n)
                def _():
                    @pl.when(j >= 1)
                    def _():
                        wait_stores(j - 1)

                    start_loads(j + 1)

                for copy in loads(j):
                    copy.wait()
                fa[b] = fa[b] + fb[b]

                @pl.when(is_mirror(r, j))
                def _():
                    fc[b] = fa[b].T
                    mirror_store(j).start()

                @pl.when(is_diag(r, j))
                def _():
                    total = fa[b]
                    at_row = lax.broadcasted_iota(jnp.int32, (TILE, TILE), 0)
                    at_col = lax.broadcasted_iota(jnp.int32, (TILE, TILE), 1)
                    fa[b] = jnp.where(at_row >= at_col, total, total.T)
                    for copy in load_packed(r):
                        copy.wait()
                    unpack(fa.at[b])

                main_store(j).start()
                return carry

            lax.fori_loop(0, n, one, 0)

            @pl.when(n >= 2)
            def _():
                wait_stores(n - 2)

            wait_stores(n - 1)

        load_res(0, 0)
        load_stm(0, 0, 0)
        enter()
        lax.fori_loop(0, n_chunk, x_start, 0)
        for k in range(1, KSTEPS):
            load_res(0, k)
            load_stm(0, 0, k)
        d2d.start()

        def strip(r, carry):
            @pl.when(r == 7)
            def _():
                remote(a.at[0], blk.at[0], s_d.at[0], r_d.at[0], y, mate).wait_recv()

            @pl.when(r == 11)
            def _():
                remote(a.at[1], blk.at[1], s_d.at[1], r_d.at[1], y, mate).wait_recv()

            @pl.when(jnp.logical_and(r >= 1, r + 1 < STRIPS))
            def _():
                for k in range(KSTEPS):
                    load_res(r + 1, k)

            n = count(r)

            def tile(j, carry):
                last = lax.div(j + 1, n)

                def before(k):
                    @pl.when(j == 0)
                    def _():
                        b = lax.rem(r, 2)
                        pltpu.make_async_copy(a.at[0, pl.ds(0, TILE), pl.ds(0, kc)], res.at[b, :, pl.ds(0, kc)], l_res.at[b * KSTEPS + k]).wait()

                def after(k):
                    @pl.when(jnp.logical_and(r == 0, j == 0))
                    def _():
                        load_res(r + 1, k)

                    @pl.when(r + last < STRIPS)
                    def _():
                        load_stm(r + last, (j + 1) * (1 - last), k)

                    @pl.when(jnp.logical_and(k == 0, jnp.logical_and(j >= 1, r + j >= 2)))
                    def _():
                        store_acc(r, j - 1).wait()
                        send(r, j - 1)

                body_steps(res.at[lax.rem(r, 2)], acc.at[lax.rem(j, 2)], False, before, after)
                store_acc(r, j).start()

                @pl.when(is_diag(r, j))
                def _():
                    pack(acc.at[lax.rem(j, 2)])
                    store_packed(r).start()

                @pl.when(jnp.logical_and(r == 0, j == 0))
                def _():
                    store_acc(r, j).wait()
                    send(r, j)

                return carry

            lax.fori_loop(0, n, tile, 0)
            store_acc(r, n - 1).wait()
            send(r, n - 1)

            @pl.when(r >= LAG)
            def _():
                finish(r - LAG)

            return carry

        lax.fori_loop(0, STRIPS, strip, 0)
        lax.fori_loop(STRIPS - LAG, STRIPS, lambda r, carry: (finish(r), carry)[1], 0)
        d2d.wait_send()
        lax.fori_loop(0, n_chunk, x_wait_send, 0)

    def cross(is_left):
        lc = 0 if is_left else 1
        mate = 0 if is_left else 3
        partner = 2 if is_left else 1
        enter()
        lax.fori_loop(0, n_chunk, x_start, 0)
        for layer in range(layers):
            remote(a.at[layer], blk.at[layer], s_d.at[layer], r_d.at[layer], y, mate).start()

        remote(a.at[lc], blk.at[0], s_d.at[0], r_d.at[0], y, mate).wait_recv()

        def region(ref, rows_first, c):
            return ref.at[at(c * CHUNK, CHUNK), :] if rows_first else ref.at[:, at(c * CHUNK, CHUNK)]

        def piece(ref, c, q):
            if is_left:
                return ref.at[at(c * CHUNK, CHUNK), at(q * TILE, TILE)]
            return ref.at[at(q * TILE, TILE), at(c * CHUNK, CHUNK)]

        def block_of(half):
            return lax.rem(half + 1 - y + 2, 2)

        def kept(b):
            return lax.rem(b + 1 - y + 2, 2)

        def load_stm(t, k):
            half, js = lax.div(t, 4), lax.rem(t, 4)
            own = block_of(half) == 1 if is_left else half == 1

            @pl.when(own)
            def _():
                pltpu.make_async_copy(a.at[lc, at(js * TILE, TILE), at(k * kc, kc)], stm.at[k], l_stm.at[k]).start()

            @pl.when(jnp.logical_not(own))
            def _():
                pltpu.make_async_copy(blk.at[0, at(js * TILE, TILE), at(k * kc, kc)], stm.at[k], l_stm.at[k]).start()

        def res_copy(c, part):
            b = lax.rem(c, 2)
            return pltpu.make_async_copy(blk.at[1 + part, at(c * CHUNK, CHUNK)], res.at[b, pl.ds(part * CHUNK, CHUNK)], l_fb.at[part])

        def acc_view(t):
            b = lax.rem(t, 2)
            return acc.at[b, pl.ds(0, 2 * CHUNK), :] if is_left else acc.at[b, :, pl.ds(0, 2 * CHUNK)]

        def store_acc(c, t):
            b, half, js = lax.rem(t, 2), lax.div(t, 4), lax.rem(t, 4)

            def views(q, dst):
                src = acc.at[b, pl.ds(q * CHUNK, CHUNK), :] if is_left else acc.at[b, :, pl.ds(q * CHUNK, CHUNK)]
                return pltpu.make_async_copy(src, piece(dst, c, js), l_acc.at[b * 2 + q])

            if is_left:
                return lambda op: (op(views(0, awy.at[half])), op(views(1, out.at[block_of(half), lc])))

            def both(op):
                @pl.when(half == 0)
                def _():
                    for q in range(2):
                        op(views(q, awy.at[kept(q)]))

                @pl.when(half == 1)
                def _():
                    for q in range(2):
                        op(views(q, out.at[q, lc]))

            return both

        def home(c, b):
            return remote(region(out.at[b, lc], is_left, c), region(prv.at[b, lc], is_left, c),
                          s_y.at[c * 2 + b], r_y.at[c * 2 + b], 1 - y, g)

        def spread(c):
            return remote(region(awy.at[0], is_left, c), region(prv.at[2, 0], is_left, c),
                          s_y.at[2 * n_chunk + c], r_y.at[2 * n_chunk + c], 1 - y, g)

        def away(c):
            return remote(region(awy.at[1], is_left, c), region(out.at[y, lc], is_left, c),
                          s_r.at[c], r_r.at[c], y, partner)

        def arrived(c):
            return remote(region(awy.at[1], not is_left, c), region(out.at[y, 1 - lc], not is_left, c),
                          s_r.at[c], r_r.at[c], y, partner)

        def away_late(c):
            return remote(pieces[0].at[c - INSIDE], late.at[c - INSIDE], s_r.at[c], r_r.at[c], y, partner)

        def gather_here(k):
            return remote(both[k].at[0], both[k].at[1], s_y.at[3 * n_chunk + k], r_y.at[3 * n_chunk + k], 1 - y, g)

        def gather(c, owner):
            here = region(out.at[owner, 1 - lc], not is_left, c)
            return remote(here, here, s_y.at[3 * n_chunk + c], r_y.at[3 * n_chunk + c], 1 - y, g)

        def add(c, local, received, store=None):
            def view(ref, q):
                return ref.at[0, pl.ds(q * CHUNK, CHUNK), :] if is_left else ref.at[0, :, pl.ds(q * CHUNK, CHUNK)]

            pairs = [(pltpu.make_async_copy(piece(local, c, q), view(fa, q), l_fa.at[q]),
                      pltpu.make_async_copy(piece(received, c, q), view(fb, q), l_fb.at[q])) for q in range(4)]
            for pair in pairs:
                for copy in pair:
                    copy.start()
            stores = [pltpu.make_async_copy(view(fa, q), piece(local, c, q), l_st.at[q]) for q in range(4)]
            for q in range(4):
                for copy in pairs[q]:
                    copy.wait()
                view(fa, q)[...] = view(fa, q)[...] + view(fb, q)[...]
                if store is None:
                    stores[q].start()
                else:
                    store(q, view(fa, q), stores[q])
            for q in range(4):
                stores[q].wait()

        def finish_away(c):
            spread(c).wait_recv()

            def store(q, total, inside):
                @pl.when(jnp.logical_and(c >= WHOLE, c < INSIDE))
                def _():
                    inside.start()

                def put(dst):
                    if is_left:
                        pltpu.make_async_copy(total, dst.at[:, pl.ds(q * TILE, TILE)], l_st.at[q]).start()
                    else:
                        for u in range(TILE // CHUNK):
                            pltpu.make_async_copy(total.at[pl.ds(u * CHUNK, CHUNK), :],
                                                  dst.at[:, pl.ds(q * TILE + u * CHUNK, CHUNK)], l_st.at[q]).start()

                for k in range(WHOLE):
                    @pl.when(c == k)
                    def _(k=k):
                        put(both[k].at[0])

                for (first, stop), piece_ref in zip(PIECES, pieces):
                    @pl.when(jnp.logical_and(c >= first, c < stop))
                    def _(first=first, piece_ref=piece_ref):
                        put(piece_ref.at[c - first])

            add(c, awy.at[1], prv.at[2, 0], store)

            for k in range(WHOLE):
                @pl.when(c == k)
                def _(k=k):
                    gather_here(k).start()

            @pl.when(jnp.logical_and(c >= WHOLE, c < INSIDE))
            def _():
                away(c).start()

            @pl.when(jnp.logical_and(c >= INSIDE, c < PIECES[0][1]))
            def _():
                away_late(c).start()

        def finish_home(c):
            for b in range(2):
                home(c, b).wait_send()
                home(c, b).wait_recv()
                add(c, out.at[b, lc], prv.at[b, lc])

        def forward(c):
            arrived(c).wait_recv()
            gather(c, y).start()

        for k in range(KSTEPS):
            load_stm(0, k)

        def compute(c):
            for part in range(2):
                remote(a.at[0, pl.ds(0, CHUNK)], blk.at[1 + part, at(c * CHUNK, CHUNK)], s_x.at[0], r_x.at[part, c], y, partner).wait_recv()
                res_copy(c, part).start()
            for part in range(2):
                res_copy(c, part).wait()

            def send_half(half):
                if is_left:
                    @pl.when(half == 0)
                    def _():
                        spread(c).start()

                    home(c, block_of(half)).start()
                else:
                    @pl.when(half == 0)
                    def _():
                        spread(c).start()

                    @pl.when(half == 1)
                    def _():
                        for b in range(2):
                            home(c, b).start()

            def tile(t, carry):
                last = lax.div(t + 1, 8)

                def after(k):
                    @pl.when(c + last < n_chunk)
                    def _():
                        load_stm((t + 1) * (1 - last), k)

                    @pl.when(jnp.logical_and(k == 0, t >= 1))
                    def _():
                        store_acc(c, t - 1)(lambda copy: copy.wait())

                        @pl.when(t == 4)
                        def _():
                            send_half(0 * t)

                        @pl.when(jnp.logical_and(c == n_chunk - 1, jnp.logical_and(lax.rem(t, 3) == 2, t < 3 * (INSIDE - WHOLE))))
                        def _():
                            forward(WHOLE + lax.div(t, 3))

                body_steps(res.at[lax.rem(c, 2), pl.ds(0, 2 * CHUNK), :], acc_view(t), not is_left, lambda k: None, after)
                store_acc(c, t)(lambda copy: copy.start())
                return carry

            lax.fori_loop(0, 8, tile, 0)
            store_acc(c, 7)(lambda copy: copy.wait())
            send_half(1 + 0 * c)

        def chunk(c, carry):
            compute(c)

            @pl.when(c >= 1)
            def _():
                finish_away(c - 1)
                finish_home(c - 1)

            return carry

        lax.fori_loop(0, n_chunk, chunk, 0)
        finish_away(n_chunk - 1)
        finish_home(n_chunk - 1)

        def drain(c, carry):
            away(c).wait_send()
            gather(c, y).wait_send()
            gather(c, 1 - y).wait_recv()
            return carry

        def drain_spread(c, carry):
            spread(c).wait_send()
            return carry

        for k in range(WHOLE):
            gather_here(k).wait_send()
            gather_here(k).wait_recv()
        lax.fori_loop(WHOLE, INSIDE, drain, 0)
        lax.fori_loop(0, n_chunk, drain_spread, 0)
        for c in range(*PIECES[0]):
            away_late(c).wait_send()
            away_late(c).wait_recv()
        for layer in range(layers):
            remote(a.at[layer], blk.at[layer], s_d.at[layer], r_d.at[layer], y, mate).wait_send()
        lax.fori_loop(0, n_chunk, x_wait_send, 0)

    pl.when(lax.rem(g, 3) == 0)(diagonal)
    pl.when(g == 1)(lambda: cross(True))
    pl.when(g == 2)(lambda: cross(False))


def assembly(step, first, *refs):
    n_in = len(first) + (step <= 2)
    ins, (out, *scratch) = refs[:n_in], refs[n_in:]
    buf, wide, l_in, l_out, l_win, l_wout = scratch
    y = lax.axis_index("kk")
    g = lax.axis_index("g")
    depth = buf.shape[0]
    lead = depth // 2

    def at(start, size):
        return pl.ds(pl.multiple_of(start, size), size)

    def copies(n, where):
        src = ins[-1]

        def view(ref, t):
            slot, layer, i, j = where(t)
            return ref.at[slot, layer, at(i * TILE, TILE), at(j * TILE, TILE)]

        def load(t):
            b = lax.rem(t, depth)
            return pltpu.make_async_copy(view(src, t), buf.at[b], l_in.at[b])

        def store(t):
            b = lax.rem(t, depth)
            return pltpu.make_async_copy(buf.at[b], view(out, t), l_out.at[b])

        def one(t, carry):
            @pl.when(jnp.logical_and(t >= depth, t < n))
            def _():
                store(t - depth).wait()

            @pl.when(t < n)
            def _():
                load(t).start()

            @pl.when(t >= lead)
            def _():
                load(t - lead).wait()
                store(t - lead).start()

            return carry

        lax.fori_loop(0, n + lead, one, 0)

        def last(t, carry):
            store(t).wait()
            return carry

        lax.fori_loop(max(n - depth, 0), n, last, 0)

    def zeros():
        buf[0] = jnp.zeros((TILE, TILE), F32)

        def store(b, layer, t):
            return pltpu.make_async_copy(buf.at[0], out.at[2, layer, at(lax.div(t, 4) * TILE, TILE), at(lax.rem(t, 4) * TILE, TILE)], l_out.at[b])

        for layer in range(2):
            for t in range(16):
                store(t, layer, t).start()
            for t in range(16):
                store(t, layer, t).wait()

    def away_results(is_left):
        layer = 1 if is_left else 0
        todo = []
        for k, ranges in enumerate(first):
            chunks = [(c, slot) for span, slot in zip(ranges, (y, 1 - y)) if span for c in range(*span)]
            todo += [(k, c, n, slot) for n, (c, slot) in enumerate(chunks)]

        def load(t):
            k, _, n, _ = todo[t]
            return pltpu.make_async_copy(ins[k].at[n], wide.at[t], l_win.at[t])

        def whole(t):
            _, c, _, slot = todo[t]
            return pltpu.make_async_copy(wide.at[t], out.at[slot, layer, pl.ds(c * CHUNK, CHUNK), :], l_wout.at[t])

        for t in range(len(todo)):
            load(t).start()
        for t in range(len(todo)):
            k, c, _, slot = todo[t]
            load(t).wait()
            if not is_left:
                whole(t).start()
            else:
                for u in range(out.shape[2] // CHUNK):
                    pltpu.make_async_copy(wide.at[t, :, pl.ds(u * CHUNK, CHUNK)],
                                          out.at[slot, layer, pl.ds(u * CHUNK, CHUNK), pl.ds(c * CHUNK, CHUNK)], l_wout.at[t]).start()
        for t in range(len(todo)):
            whole(t).wait()

    def on_cross(is_left):
        lc = 0 if is_left else 1
        away_results(is_left)
        if step == 0:
            if is_left:
                copies(8, lambda t: (lax.div(t, 4), 1 - lc, lax.rem(t, 4), 0))
            else:
                copies(8, lambda t: (lax.div(t, 4), 1 - lc, 0, lax.rem(t, 4)))
        elif step <= 2:
            copies(16, lambda t: (step - 1, lc, lax.div(t, 4), lax.rem(t, 4)))
            if step == 2:
                zeros()

    @pl.when(g == 1)
    def _():
        on_cross(True)

    @pl.when(g == 2)
    def _():
        on_cross(False)

    if step < 3:
        @pl.when(lax.rem(g, 3) == 0)
        def _():
            copies(32, lambda t: (step, lax.div(t, 16), lax.div(lax.rem(t, 16), 4), lax.rem(t, 4)))


def solution(mesh):
    assert dict(mesh.shape) == {"m": 1, "kk": 2, "g": 4}
    dma = pltpu.SemaphoreType.DMA

    def local_part(a_loc):
        layers, rows, cols = a_loc.shape
        n_chunk = rows // CHUNK
        any_space = pl.BlockSpec(memory_space=pl.ANY)
        slots_shape = jax.ShapeDtypeStruct((3, layers, rows, rows), F32)

        def chunks_shape(n):
            return jax.ShapeDtypeStruct((n, CHUNK, rows), F32)

        slots, _, _, _, _, _, late, *others = pl.pallas_call(
            kernel,
            out_shape=(
                slots_shape,
                jax.ShapeDtypeStruct((3, rows, cols), a_loc.dtype),
                slots_shape,
                jax.ShapeDtypeStruct((2, rows, rows), F32),
                jax.ShapeDtypeStruct((16, PACKED, 128), F32),
                jax.ShapeDtypeStruct((16, PACKED, 128), F32),
                chunks_shape(PIECES[0][1] - PIECES[0][0]),
                *(chunks_shape(2) for _ in range(WHOLE)),
                *(chunks_shape(stop - start) for start, stop in PIECES),
            ),
            in_specs=[any_space],
            out_specs=(any_space,) * (7 + WHOLE + len(PIECES)),
            scratch_shapes=[
                pltpu.VMEM((2, TILE, cols), a_loc.dtype),
                pltpu.VMEM((KSTEPS, TILE, cols // KSTEPS), a_loc.dtype),
                pltpu.VMEM((2, TILE, TILE), F32),
                pltpu.VMEM((2, TILE, TILE), F32),
                pltpu.VMEM((2, TILE, TILE), F32),
                pltpu.VMEM((2, TILE, TILE), F32),
                pltpu.VMEM((PACKED, 128), F32),
                pltpu.VMEM((PACKED, 128), F32),
                pltpu.VMEM((PACKED, 128), F32),
                dma((n_chunk,)), dma((2, n_chunk)), dma((2,)), dma((2,)),
                dma((4 * n_chunk,)), dma((4 * STRIPS + 16,)), dma((n_chunk,)), dma((n_chunk,)),
                dma((2 * KSTEPS,)), dma((KSTEPS,)), dma((4,)), dma((4,)), dma((4,)), dma((4,)), dma((2,)), dma((3,)),
            ],
            compiler_params=pltpu.CompilerParams(
                collective_id=0, has_side_effects=True, vmem_limit_bytes=63 * 2**20),
            cost_estimate=pl.CostEstimate(flops=10**12, bytes_accessed=10**9, transcendentals=0),
        )(a_loc)

        both, pieces = others[:WHOLE], others[WHOLE:]
        other_chip = [(1, 2), (2, 1)]
        other_half = [(1, 5), (5, 1), (2, 6), (6, 2)]

        n_pieces = len(PIECES)
        mine = [late] + [lax.ppermute(pieces[k], "g", other_chip) for k in range(1, n_pieces)]
        theirs = [lax.ppermute(mine[k], ("kk", "g"), other_half) for k in range(n_pieces)]
        pairs = [lax.ppermute(both[k], "g", other_chip) for k in range(WHOLE)]

        def assemble(step, result, parts):
            first = tuple(((k, k + 1),) * 2 if kind == "pair" else (PIECES[k], None) if kind == "mine" else (None, PIECES[k])
                          for kind, k in parts)
            arrays = [{"mine": mine, "theirs": theirs, "pair": pairs}[kind][k] for kind, k in parts]
            n_wide = max(1, sum(stop - start for ranges in first for start, stop in filter(None, ranges)))
            sources = arrays + ([slots] if step <= 2 else [])
            aliases = {}
            operands = sources
            if step > 0:
                operands = [result] + sources
                aliases = {0: 0}

            def body(*refs):
                assembly(step, first, *refs[len(operands) - len(sources):])

            return pl.pallas_call(
                body,
                out_shape=slots_shape,
                in_specs=[any_space] * len(operands),
                out_specs=any_space,
                input_output_aliases=aliases,
                scratch_shapes=[
                    pltpu.VMEM((16, TILE, TILE), F32), pltpu.VMEM((n_wide, CHUNK, rows), F32),
                    dma((16,)), dma((16,)), dma((n_wide,)), dma((n_wide,)),
                ],
                compiler_params=pltpu.CompilerParams(vmem_limit_bytes=67043328),
                cost_estimate=pl.CostEstimate(flops=10**10, bytes_accessed=10**8, transcendentals=0),
            )(*operands)

        result = assemble(0, None, [])
        result = assemble(1, result, [("mine", 0)])
        result = assemble(2, result, [("mine", 1)])
        result = assemble(3, result, [("mine", 2), ("theirs", 0)])
        result = assemble(4, result, [("mine", 3), ("theirs", 1)])
        result = assemble(5, result, [("pair", 0), ("theirs", 2)])
        result = assemble(6, result, [("pair", 1), ("theirs", 3)])
        return result[None]

    return jax.shard_map(local_part, mesh=mesh, in_specs=(P(None, ("m", "g"), "kk"),),
                         out_specs=P(("m", "g"), None, None, None, None), check_vma=False)
```

```python
import jax
import jax.numpy as jnp
from jax import lax
from jax.experimental import pallas as pl
from jax.experimental.pallas import tpu as pltpu
from jax.sharding import PartitionSpec as P


MESH = pl.DeviceIdType.MESH
NT = (((1,), (1,)), ((), ()))
F32 = jnp.float32

SQUARE = 128
TILE = 512
CHUNK = 128
STRIPS = 24
KSTEPS = 2
LAG = 4
PACKED = 264
WHOLE = 2
INSIDE = 4
PIECES = ((4, 8), (8, 11), (11, 14), (14, 16))


def half_of(value):
    return lax.rem(value, 2)


def kernel(a, out, blk, prv, awy, pkl, pkr, late, *refs):
    both, pieces, refs = refs[:WHOLE], refs[WHOLE:WHOLE + len(PIECES)], refs[WHOLE + len(PIECES):]
    work(a, out, blk, prv, awy, pkl, pkr, late, both, pieces, *refs)


def work(a, out, blk, prv, awy, pkl, pkr, late, both, pieces, res, stm, acc, fa, fb, fc, pk, fpa, fpb,
         s_x, r_x, s_d, r_d, s_y, r_y, s_r, r_r,
         l_res, l_stm, l_acc, l_fa, l_fb, l_st, l_tr, l_pk):
    m = lax.axis_index("m")
    y = lax.axis_index("kk")
    g = lax.axis_index("g")
    side = lax.div(g, 2)
    layers, rows, cols = a.shape
    kc = cols // KSTEPS
    n_strip = rows // TILE
    n_chunk = rows // CHUNK

    def at(start, size):
        return pl.ds(pl.multiple_of(start, size), size)

    def remote(src, dst, ss, rs, kk2, g2):
        return pltpu.make_async_remote_copy(src, dst, ss, rs, device_id=(m, kk2, g2), device_id_type=MESH)

    def enter():
        barrier = pltpu.get_barrier_semaphore()
        me = y * 4 + g
        for step in range(1, 8):
            other = lax.rem(me + step, 8)
            pl.semaphore_signal(barrier, inc=1, device_id=(m, lax.div(other, 4), lax.rem(other, 4)), device_id_type=MESH)
        pl.semaphore_wait(barrier, 7)

    def x_in(c):
        part = half_of(g)
        return remote(a.at[1 - side, at(c * CHUNK, CHUNK)], blk.at[1 + part, at(c * CHUNK, CHUNK)],
                      s_x.at[c], r_x.at[part, c], y, 2 - side)

    def x_start(c, carry):
        x_in(c).start()
        return carry

    def x_wait_send(c, carry):
        x_in(c).wait_send()
        return carry

    def body_steps(res_view, acc_view, swap, before, after):
        acc_view[...] = jnp.zeros(acc_view.shape, F32)

        def step(k, carry):
            before(k)
            pltpu.make_async_copy(a.at[0, pl.ds(0, TILE), pl.ds(0, kc)], stm.at[k], l_stm.at[k]).wait()
            lhs = res_view[:, at(k * kc, kc)]
            rhs = stm[k]
            if swap:
                lhs, rhs = rhs, lhs
            acc_view[...] += lax.dot_general(lhs, rhs, NT, preferred_element_type=F32)
            after(k)
            return carry

        lax.fori_loop(0, KSTEPS, step, 0)

    def diagonal():
        d = lax.div(g, 3)
        mate = g + 1 - 2 * d
        d2d = remote(a.at[side], blk.at[0], s_d.at[0], r_d.at[0], y, mate)

        def phase(r):
            return lax.div(r, 8), lax.rem(lax.div(r, 4), 2), n_strip - 1 - lax.rem(r, 4)

        def count(r):
            p, _, i = phase(r)
            return (i + 1) + half_of(p) * (n_strip - 1 - i)

        def slot(p):
            return p * (1 - 2 * d) + 2 * d

        def load(own, layer, row, col, width, dst, sem):
            @pl.when(own)
            def _():
                pltpu.make_async_copy(a.at[layer, at(row, TILE), at(col, width)], dst, sem).start()

            @pl.when(jnp.logical_not(own))
            def _():
                pltpu.make_async_copy(blk.at[layer, at(row, TILE), at(col, width)], dst, sem).start()

        def load_res(r, k):
            p, layer, i = phase(r)
            own = p + 1 - d < 2
            load(own, layer, i * TILE, k * kc, kc, res.at[half_of(r), :, at(k * kc, kc)], l_res.at[half_of(r) * KSTEPS + k])

        def load_stm(r, j, k):
            p, layer, _ = phase(r)
            own = p + d < 2
            load(own, layer, j * TILE, k * kc, kc, stm.at[k], l_stm.at[k])

        def tile_of(ref, r, i, j):
            p, layer, _ = phase(r)
            return ref.at[slot(p), layer, at(i * TILE, TILE), at(j * TILE, TILE)]

        def is_diag(r, j):
            p, _, i = phase(r)
            return jnp.logical_and(p != 1, i == j)

        def is_mirror(r, j):
            p, _, i = phase(r)
            return jnp.logical_and(p != 1, i != j)

        def whole(r, j):
            i = phase(r)[2]
            return remote(tile_of(out, r, i, j), tile_of(prv, r, i, j),
                          s_y.at[lax.rem(r, 8) * 4 + j], r_y.at[r * 4 + j], 1 - y, g)

        def lower(r, j, row, height, width):
            p, layer, i = phase(r)

            def part(ref):
                return ref.at[slot(p), layer, pl.ds(pl.multiple_of(i * TILE + row, SQUARE), height), pl.ds(pl.multiple_of(j * TILE, TILE), width)]

            return remote(part(out), part(prv), s_y.at[lax.rem(r, 8) * 4 + j], r_y.at[r * 4 + j], 1 - y, g)

        def packed_no(r):
            return lax.rem(r, 8) + 8 * lax.div(phase(r)[0], 2)

        def packed(r):
            e = packed_no(r)
            return remote(pkl.at[e], pkr.at[e], s_y.at[32 + lax.rem(r, 8)], r_y.at[4 * STRIPS + e], 1 - y, g)

        def store_packed(r):
            return pltpu.make_async_copy(pk, pkl.at[packed_no(r)], l_pk.at[0])

        def load_packed(r):
            e = packed_no(r)
            return pltpu.make_async_copy(pkl.at[e], fpa, l_pk.at[1]), pltpu.make_async_copy(pkr.at[e], fpb, l_pk.at[2])

        row_id = lax.broadcasted_iota(jnp.int32, (SQUARE, SQUARE), 0)
        col_id = lax.broadcasted_iota(jnp.int32, (SQUARE, SQUARE), 1)

        def square(ref, k):
            span = pl.ds(SQUARE * k, SQUARE)
            return ref.at[span, span]

        def pack(tile):
            ends = []
            for h in range(2):
                first, second = square(tile, 2 * h)[...], square(tile, 2 * h + 1)[...]
                pk[pl.ds(SQUARE * h, SQUARE), :] = jnp.where(row_id > col_id, first, second.T)
                ends.append(jnp.sum(jnp.where(row_id == col_id, first, 0.0), axis=0, keepdims=True))
            pk[pl.ds(2 * SQUARE, 8), :] = jnp.where(row_id[:8] == 0, *ends)

        def unpack(tile):
            fpa[...] = fpa[...] + fpb[...]
            for h in range(2):
                shared = fpa[pl.ds(SQUARE * h, SQUARE), :]
                turned = shared.T
                ends = fpa[pl.ds(2 * SQUARE + h, 1), :]
                square(tile, 2 * h)[...] = jnp.where(row_id > col_id, shared, jnp.where(row_id == col_id, ends, turned))
                square(tile, 2 * h + 1)[...] = jnp.where(row_id <= col_id, shared, turned)

        def send(r, j):
            @pl.when(is_diag(r, j))
            def _():
                for row in range(SQUARE, TILE, SQUARE):
                    lower(r, j, row, SQUARE, row).start()
                store_packed(r).wait()
                packed(r).start()

            @pl.when(jnp.logical_not(is_diag(r, j)))
            def _():
                whole(r, j).start()

        def wait_exchange(r, j):
            @pl.when(is_diag(r, j))
            def _():
                sized = lower(r, j, 0, 3 * SQUARE // 2, TILE)
                sized.wait_send()
                sized.wait_recv()
                packed(r).wait_send()
                packed(r).wait_recv()

            @pl.when(jnp.logical_not(is_diag(r, j)))
            def _():
                whole(r, j).wait_send()
                whole(r, j).wait_recv()

        def store_acc(r, j):
            return pltpu.make_async_copy(acc.at[half_of(j)], tile_of(out, r, phase(r)[2], j), l_acc.at[half_of(j)])

        def finish(r):
            n = count(r)
            i = phase(r)[2]

            def loads(j):
                b = half_of(j)
                return (pltpu.make_async_copy(tile_of(out, r, i, j), fa.at[b], l_fa.at[b]),
                        pltpu.make_async_copy(tile_of(prv, r, i, j), fb.at[b], l_fb.at[b]))

            def start_loads(j):
                wait_exchange(r, j)
                for copy in loads(j):
                    copy.start()

                @pl.when(is_diag(r, j))
                def _():
                    for copy in load_packed(r):
                        copy.start()

            def main_store(j):
                return pltpu.make_async_copy(fa.at[half_of(j)], tile_of(out, r, i, j), l_st.at[half_of(j)])

            def mirror_store(j):
                return pltpu.make_async_copy(fc.at[half_of(j)], tile_of(out, r, j, i), l_tr.at[half_of(j)])

            def wait_stores(j):
                main_store(j).wait()

                @pl.when(is_mirror(r, j))
                def _():
                    mirror_store(j).wait()

            start_loads(0)

            def one(j, carry):
                b = half_of(j)

                @pl.when(j + 1 < n)
                def _():
                    @pl.when(j >= 1)
                    def _():
                        wait_stores(j - 1)

                    start_loads(j + 1)

                for copy in loads(j):
                    copy.wait()
                fa[b] = fa[b] + fb[b]

                @pl.when(is_mirror(r, j))
                def _():
                    fc[b] = fa[b].T
                    mirror_store(j).start()

                @pl.when(is_diag(r, j))
                def _():
                    total = fa[b]
                    at_row = lax.broadcasted_iota(jnp.int32, (TILE, TILE), 0)
                    at_col = lax.broadcasted_iota(jnp.int32, (TILE, TILE), 1)
                    fa[b] = jnp.where(at_row >= at_col, total, total.T)
                    for copy in load_packed(r):
                        copy.wait()
                    unpack(fa.at[b])

                main_store(j).start()
                return carry

            lax.fori_loop(0, n, one, 0)

            @pl.when(n >= 2)
            def _():
                wait_stores(n - 2)

            wait_stores(n - 1)

        load_res(0, 0)
        load_stm(0, 0, 0)
        enter()
        lax.fori_loop(0, n_chunk, x_start, 0)
        for k in range(1, KSTEPS):
            load_res(0, k)
            load_stm(0, 0, k)
        d2d.start()

        def strip(r, carry):
            @pl.when(r == 7)
            def _():
                remote(a.at[0], blk.at[0], s_d.at[0], r_d.at[0], y, mate).wait_recv()

            @pl.when(r == 11)
            def _():
                remote(a.at[1], blk.at[1], s_d.at[1], r_d.at[1], y, mate).wait_recv()

            @pl.when(jnp.logical_and(r >= 1, r + 1 < STRIPS))
            def _():
                for k in range(KSTEPS):
                    load_res(r + 1, k)

            n = count(r)

            def tile(j, carry):
                last = lax.div(j + 1, n)

                def before(k):
                    @pl.when(j == 0)
                    def _():
                        b = half_of(r)
                        pltpu.make_async_copy(a.at[0, pl.ds(0, TILE), pl.ds(0, kc)], res.at[b, :, pl.ds(0, kc)], l_res.at[b * KSTEPS + k]).wait()

                def after(k):
                    @pl.when(jnp.logical_and(r == 0, j == 0))
                    def _():
                        load_res(r + 1, k)

                    @pl.when(r + last < STRIPS)
                    def _():
                        load_stm(r + last, (j + 1) * (1 - last), k)

                    @pl.when(jnp.logical_and(k == 0, jnp.logical_and(j >= 1, r + j >= 2)))
                    def _():
                        store_acc(r, j - 1).wait()
                        send(r, j - 1)

                body_steps(res.at[half_of(r)], acc.at[half_of(j)], False, before, after)
                store_acc(r, j).start()

                @pl.when(is_diag(r, j))
                def _():
                    pack(acc.at[half_of(j)])
                    store_packed(r).start()

                @pl.when(jnp.logical_and(r == 0, j == 0))
                def _():
                    store_acc(r, j).wait()
                    send(r, j)

                return carry

            lax.fori_loop(0, n, tile, 0)
            store_acc(r, n - 1).wait()
            send(r, n - 1)

            @pl.when(r >= LAG)
            def _():
                finish(r - LAG)

            return carry

        lax.fori_loop(0, STRIPS, strip, 0)
        lax.fori_loop(STRIPS - LAG, STRIPS, lambda r, carry: (finish(r), carry)[1], 0)
        d2d.wait_send()
        lax.fori_loop(0, n_chunk, x_wait_send, 0)

    def cross(is_left):
        lc = 0 if is_left else 1
        mate = 0 if is_left else 3
        partner = 2 if is_left else 1
        enter()
        lax.fori_loop(0, n_chunk, x_start, 0)
        for layer in range(layers):
            remote(a.at[layer], blk.at[layer], s_d.at[layer], r_d.at[layer], y, mate).start()

        remote(a.at[lc], blk.at[0], s_d.at[0], r_d.at[0], y, mate).wait_recv()

        def region(ref, rows_first, c):
            return ref.at[at(c * CHUNK, CHUNK), :] if rows_first else ref.at[:, at(c * CHUNK, CHUNK)]

        def piece(ref, c, q):
            if is_left:
                return ref.at[at(c * CHUNK, CHUNK), at(q * TILE, TILE)]
            return ref.at[at(q * TILE, TILE), at(c * CHUNK, CHUNK)]

        def block_of(half):
            return lax.rem(half + 1 - y + 2, 2)

        def kept(b):
            return lax.rem(b + 1 - y + 2, 2)

        def load_stm(t, k):
            half, js = lax.div(t, 4), lax.rem(t, 4)
            own = block_of(half) == 1 if is_left else half == 1

            @pl.when(own)
            def _():
                pltpu.make_async_copy(a.at[lc, at(js * TILE, TILE), at(k * kc, kc)], stm.at[k], l_stm.at[k]).start()

            @pl.when(jnp.logical_not(own))
            def _():
                pltpu.make_async_copy(blk.at[0, at(js * TILE, TILE), at(k * kc, kc)], stm.at[k], l_stm.at[k]).start()

        def res_copy(c, part):
            b = half_of(c)
            return pltpu.make_async_copy(blk.at[1 + part, at(c * CHUNK, CHUNK)], res.at[b, pl.ds(part * CHUNK, CHUNK)], l_fb.at[part])

        def acc_view(t):
            b = half_of(t)
            return acc.at[b, pl.ds(0, 2 * CHUNK), :] if is_left else acc.at[b, :, pl.ds(0, 2 * CHUNK)]

        def store_acc(c, t):
            b, half, js = half_of(t), lax.div(t, 4), lax.rem(t, 4)

            def views(q, dst):
                src = acc.at[b, pl.ds(q * CHUNK, CHUNK), :] if is_left else acc.at[b, :, pl.ds(q * CHUNK, CHUNK)]
                return pltpu.make_async_copy(src, piece(dst, c, js), l_acc.at[b * 2 + q])

            if is_left:
                return lambda op: (op(views(0, awy.at[half])), op(views(1, out.at[block_of(half), lc])))

            def both(op):
                @pl.when(half == 0)
                def _():
                    for q in range(2):
                        op(views(q, awy.at[kept(q)]))

                @pl.when(half == 1)
                def _():
                    for q in range(2):
                        op(views(q, out.at[q, lc]))

            return both

        def home(c, b):
            return remote(region(out.at[b, lc], is_left, c), region(prv.at[b, lc], is_left, c),
                          s_y.at[c * 2 + b], r_y.at[c * 2 + b], 1 - y, g)

        def spread(c):
            return remote(region(awy.at[0], is_left, c), region(prv.at[2, 0], is_left, c),
                          s_y.at[2 * n_chunk + c], r_y.at[2 * n_chunk + c], 1 - y, g)

        def away(c):
            return remote(region(awy.at[1], is_left, c), region(out.at[y, lc], is_left, c),
                          s_r.at[c], r_r.at[c], y, partner)

        def arrived(c):
            return remote(region(awy.at[1], not is_left, c), region(out.at[y, 1 - lc], not is_left, c),
                          s_r.at[c], r_r.at[c], y, partner)

        def away_late(c):
            return remote(pieces[0].at[c - INSIDE], late.at[c - INSIDE], s_r.at[c], r_r.at[c], y, partner)

        def gather_here(k):
            return remote(both[k].at[0], both[k].at[1], s_y.at[3 * n_chunk + k], r_y.at[3 * n_chunk + k], 1 - y, g)

        def gather(c, owner):
            here = region(out.at[owner, 1 - lc], not is_left, c)
            return remote(here, here, s_y.at[3 * n_chunk + c], r_y.at[3 * n_chunk + c], 1 - y, g)

        def add(c, local, received, store=None):
            def view(ref, q):
                return ref.at[0, pl.ds(q * CHUNK, CHUNK), :] if is_left else ref.at[0, :, pl.ds(q * CHUNK, CHUNK)]

            pairs = [(pltpu.make_async_copy(piece(local, c, q), view(fa, q), l_fa.at[q]),
                      pltpu.make_async_copy(piece(received, c, q), view(fb, q), l_fb.at[q])) for q in range(4)]
            for pair in pairs:
                for copy in pair:
                    copy.start()
            stores = [pltpu.make_async_copy(view(fa, q), piece(local, c, q), l_st.at[q]) for q in range(4)]
            for q in range(4):
                for copy in pairs[q]:
                    copy.wait()
                view(fa, q)[...] = view(fa, q)[...] + view(fb, q)[...]
                if store is None:
                    stores[q].start()
                else:
                    store(q, view(fa, q), stores[q])
            for q in range(4):
                stores[q].wait()

        def finish_away(c):
            spread(c).wait_recv()

            def store(q, total, inside):
                @pl.when(jnp.logical_and(c >= WHOLE, c < INSIDE))
                def _():
                    inside.start()

                def put(dst):
                    if is_left:
                        pltpu.make_async_copy(total, dst.at[:, pl.ds(q * TILE, TILE)], l_st.at[q]).start()
                    else:
                        for u in range(TILE // CHUNK):
                            pltpu.make_async_copy(total.at[pl.ds(u * CHUNK, CHUNK), :],
                                                  dst.at[:, pl.ds(q * TILE + u * CHUNK, CHUNK)], l_st.at[q]).start()

                for k in range(WHOLE):
                    @pl.when(c == k)
                    def _(k=k):
                        put(both[k].at[0])

                for (first, stop), piece_ref in zip(PIECES, pieces):
                    @pl.when(jnp.logical_and(c >= first, c < stop))
                    def _(first=first, piece_ref=piece_ref):
                        put(piece_ref.at[c - first])

            add(c, awy.at[1], prv.at[2, 0], store)

            for k in range(WHOLE):
                @pl.when(c == k)
                def _(k=k):
                    gather_here(k).start()

            @pl.when(jnp.logical_and(c >= WHOLE, c < INSIDE))
            def _():
                away(c).start()

            @pl.when(jnp.logical_and(c >= INSIDE, c < PIECES[0][1]))
            def _():
                away_late(c).start()

        def finish_home(c):
            for b in range(2):
                home(c, b).wait_send()
                home(c, b).wait_recv()
                add(c, out.at[b, lc], prv.at[b, lc])

        def forward(c):
            arrived(c).wait_recv()
            gather(c, y).start()

        for k in range(KSTEPS):
            load_stm(0, k)

        def compute(c):
            for part in range(2):
                remote(a.at[0, pl.ds(0, CHUNK)], blk.at[1 + part, at(c * CHUNK, CHUNK)], s_x.at[0], r_x.at[part, c], y, partner).wait_recv()
                res_copy(c, part).start()
            for part in range(2):
                res_copy(c, part).wait()

            def send_half(half):
                if is_left:
                    @pl.when(half == 0)
                    def _():
                        spread(c).start()

                    home(c, block_of(half)).start()
                else:
                    @pl.when(half == 0)
                    def _():
                        spread(c).start()

                    @pl.when(half == 1)
                    def _():
                        for b in range(2):
                            home(c, b).start()

            def tile(t, carry):
                last = lax.div(t + 1, 8)

                def after(k):
                    @pl.when(c + last < n_chunk)
                    def _():
                        load_stm((t + 1) * (1 - last), k)

                    @pl.when(jnp.logical_and(k == 0, t >= 1))
                    def _():
                        store_acc(c, t - 1)(lambda copy: copy.wait())

                        @pl.when(t == 4)
                        def _():
                            send_half(0 * t)

                        @pl.when(jnp.logical_and(c == n_chunk - 1, lax.rem(t, 3) == 2))
                        def _():
                            forward(WHOLE + lax.div(t, 3))

                body_steps(res.at[half_of(c), pl.ds(0, 2 * CHUNK), :], acc_view(t), not is_left, lambda k: None, after)
                store_acc(c, t)(lambda copy: copy.start())
                return carry

            lax.fori_loop(0, 8, tile, 0)
            store_acc(c, 7)(lambda copy: copy.wait())
            send_half(1 + 0 * c)

        def chunk(c, carry):
            compute(c)

            @pl.when(c >= 1)
            def _():
                finish_away(c - 1)
                finish_home(c - 1)

            return carry

        lax.fori_loop(0, n_chunk, chunk, 0)
        finish_away(n_chunk - 1)
        finish_home(n_chunk - 1)

        def drain(c, carry):
            away(c).wait_send()
            gather(c, y).wait_send()
            gather(c, 1 - y).wait_recv()
            return carry

        def drain_spread(c, carry):
            spread(c).wait_send()
            return carry

        for k in range(WHOLE):
            gather_here(k).wait_send()
            gather_here(k).wait_recv()
        lax.fori_loop(WHOLE, INSIDE, drain, 0)
        lax.fori_loop(0, n_chunk, drain_spread, 0)
        for c in range(*PIECES[0]):
            away_late(c).wait_send()
            away_late(c).wait_recv()
        for layer in range(layers):
            remote(a.at[layer], blk.at[layer], s_d.at[layer], r_d.at[layer], y, mate).wait_send()
        lax.fori_loop(0, n_chunk, x_wait_send, 0)

    pl.when(lax.rem(g, 3) == 0)(diagonal)
    pl.when(g == 1)(lambda: cross(True))
    pl.when(g == 2)(lambda: cross(False))


def assembly(step, first, *refs):
    n_in = len(first) + (step <= 2)
    ins, (out, *scratch) = refs[:n_in], refs[n_in:]
    buf, wide, l_in, l_out, l_win, l_wout = scratch
    y = lax.axis_index("kk")
    g = lax.axis_index("g")
    depth = buf.shape[0]
    lead = depth // 2

    def at(start, size):
        return pl.ds(pl.multiple_of(start, size), size)

    def copies(n, where):
        src = ins[-1]

        def view(ref, t):
            slot, layer, i, j = where(t)
            return ref.at[slot, layer, at(i * TILE, TILE), at(j * TILE, TILE)]

        def load(t):
            b = lax.rem(t, depth)
            return pltpu.make_async_copy(view(src, t), buf.at[b], l_in.at[b])

        def store(t):
            b = lax.rem(t, depth)
            return pltpu.make_async_copy(buf.at[b], view(out, t), l_out.at[b])

        def one(t, carry):
            @pl.when(jnp.logical_and(t >= depth, t < n))
            def _():
                store(t - depth).wait()

            @pl.when(t < n)
            def _():
                load(t).start()

            @pl.when(t >= lead)
            def _():
                load(t - lead).wait()
                store(t - lead).start()

            return carry

        lax.fori_loop(0, n + lead, one, 0)

        def last(t, carry):
            store(t).wait()
            return carry

        lax.fori_loop(max(n - depth, 0), n, last, 0)

    def zeros():
        buf[0] = jnp.zeros((TILE, TILE), F32)

        def store(b, layer, t):
            return pltpu.make_async_copy(buf.at[0], out.at[2, layer, at(lax.div(t, 4) * TILE, TILE), at(lax.rem(t, 4) * TILE, TILE)], l_out.at[b])

        for layer in range(2):
            for t in range(16):
                store(t, layer, t).start()
            for t in range(16):
                store(t, layer, t).wait()

    def away_results(is_left):
        layer = 1 if is_left else 0
        todo = []
        for k, ranges in enumerate(first):
            chunks = [(c, slot) for span, slot in zip(ranges, (y, 1 - y)) if span for c in range(*span)]
            todo += [(k, c, n, slot) for n, (c, slot) in enumerate(chunks)]

        def load(t):
            k, _, n, _ = todo[t]
            return pltpu.make_async_copy(ins[k].at[n], wide.at[t], l_win.at[t])

        def whole(t):
            _, c, _, slot = todo[t]
            return pltpu.make_async_copy(wide.at[t], out.at[slot, layer, pl.ds(c * CHUNK, CHUNK), :], l_wout.at[t])

        for t in range(len(todo)):
            load(t).start()
        for t in range(len(todo)):
            k, c, _, slot = todo[t]
            load(t).wait()
            if not is_left:
                whole(t).start()
            else:
                for u in range(out.shape[2] // CHUNK):
                    pltpu.make_async_copy(wide.at[t, :, pl.ds(u * CHUNK, CHUNK)],
                                          out.at[slot, layer, pl.ds(u * CHUNK, CHUNK), pl.ds(c * CHUNK, CHUNK)], l_wout.at[t]).start()
        for t in range(len(todo)):
            whole(t).wait()

    def on_cross(is_left):
        lc = 0 if is_left else 1
        away_results(is_left)
        if step == 0:
            if is_left:
                copies(8, lambda t: (lax.div(t, 4), 1 - lc, lax.rem(t, 4), 0))
            else:
                copies(8, lambda t: (lax.div(t, 4), 1 - lc, 0, lax.rem(t, 4)))
        elif step <= 2:
            copies(16, lambda t: (step - 1, lc, lax.div(t, 4), lax.rem(t, 4)))
            if step == 2:
                zeros()

    @pl.when(g == 1)
    def _():
        on_cross(True)

    @pl.when(g == 2)
    def _():
        on_cross(False)

    if step < 3:
        @pl.when(lax.rem(g, 3) == 0)
        def _():
            copies(32, lambda t: (step, lax.div(t, 16), lax.div(lax.rem(t, 16), 4), lax.rem(t, 4)))


def solution(mesh):
    assert dict(mesh.shape) == {"m": 1, "kk": 2, "g": 4}
    dma = pltpu.SemaphoreType.DMA

    def local_part(a_loc):
        layers, rows, cols = a_loc.shape
        n_chunk = rows // CHUNK
        any_space = pl.BlockSpec(memory_space=pl.ANY)
        slots_shape = jax.ShapeDtypeStruct((3, layers, rows, rows), F32)

        def chunks_shape(n):
            return jax.ShapeDtypeStruct((n, CHUNK, rows), F32)

        slots, _, _, _, _, _, late, *others = pl.pallas_call(
            kernel,
            out_shape=(
                slots_shape,
                jax.ShapeDtypeStruct((3, rows, cols), a_loc.dtype),
                slots_shape,
                jax.ShapeDtypeStruct((2, rows, rows), F32),
                *(jax.ShapeDtypeStruct((16, PACKED, SQUARE), F32) for _ in range(2)),
                chunks_shape(PIECES[0][1] - PIECES[0][0]),
                *(chunks_shape(2) for _ in range(WHOLE)),
                *(chunks_shape(stop - start) for start, stop in PIECES),
            ),
            in_specs=[any_space],
            out_specs=(any_space,) * (7 + WHOLE + len(PIECES)),
            scratch_shapes=[
                pltpu.VMEM((2, TILE, cols), a_loc.dtype),
                pltpu.VMEM((KSTEPS, TILE, cols // KSTEPS), a_loc.dtype),
                *[pltpu.VMEM((2, TILE, TILE), F32)] * 4,
                *[pltpu.VMEM((PACKED, SQUARE), F32)] * 3,
                dma((n_chunk,)), dma((2, n_chunk)), dma((2,)), dma((2,)),
                dma((4 * n_chunk,)), dma((4 * STRIPS + 16,)), dma((n_chunk,)), dma((n_chunk,)),
                dma((2 * KSTEPS,)), dma((KSTEPS,)), *[dma((4,))] * 6,
            ],
            compiler_params=pltpu.CompilerParams(
                collective_id=0, has_side_effects=True, vmem_limit_bytes=63 * 2**20),
            cost_estimate=pl.CostEstimate(flops=10**12, bytes_accessed=10**9, transcendentals=0),
        )(a_loc)

        both, pieces = others[:WHOLE], others[WHOLE:]
        other_chip = [(1, 2), (2, 1)]
        other_half = [(1, 5), (5, 1), (2, 6), (6, 2)]

        n_pieces = len(PIECES)
        mine = [late] + [lax.ppermute(pieces[k], "g", other_chip) for k in range(1, n_pieces)]
        theirs = [lax.ppermute(mine[k], ("kk", "g"), other_half) for k in range(n_pieces)]
        pairs = [lax.ppermute(both[k], "g", other_chip) for k in range(WHOLE)]

        def assemble(step, result, parts):
            first = tuple(((k, k + 1),) * 2 if kind == "pair" else (PIECES[k], None) if kind == "mine" else (None, PIECES[k])
                          for kind, k in parts)
            arrays = [{"mine": mine, "theirs": theirs, "pair": pairs}[kind][k] for kind, k in parts]
            n_wide = max(1, sum(stop - start for ranges in first for start, stop in filter(None, ranges)))
            sources = arrays + ([slots] if step <= 2 else [])
            aliases = {}
            operands = sources
            if step > 0:
                operands = [result] + sources
                aliases = {0: 0}

            def body(*refs):
                assembly(step, first, *refs[len(operands) - len(sources):])

            return pl.pallas_call(
                body,
                out_shape=slots_shape,
                in_specs=[any_space] * len(operands),
                out_specs=any_space,
                input_output_aliases=aliases,
                scratch_shapes=[
                    pltpu.VMEM((16, TILE, TILE), F32), pltpu.VMEM((n_wide, CHUNK, rows), F32),
                    dma((16,)), dma((16,)), dma((n_wide,)), dma((n_wide,)),
                ],
                compiler_params=pltpu.CompilerParams(vmem_limit_bytes=67043328),
                cost_estimate=pl.CostEstimate(flops=10**10, bytes_accessed=10**8, transcendentals=0),
            )(*operands)

        result = assemble(0, None, [])
        for step in range(1, n_pieces + WHOLE + 1):
            own, other = step - 1, step - WHOLE - 1
            parts = [("mine", own) if own < n_pieces else ("pair", own - n_pieces)]
            result = assemble(step, result, parts + ([("theirs", other)] if other >= 0 else []))
        return result[None]

    return jax.shard_map(local_part, mesh=mesh, in_specs=(P(None, ("m", "g"), "kk"),),
                         out_specs=P(("m", "g"), None, None, None, None), check_vma=False)
```

```python
import jax
import jax.numpy as jnp
from jax import lax
from jax.experimental import pallas as pl
from jax.experimental.pallas import tpu as pltpu
from jax.sharding import PartitionSpec as P


MESH = pl.DeviceIdType.MESH
NT = (((1,), (1,)), ((), ()))
F32 = jnp.float32

SQUARE = 128
TILE = 512
CHUNK = 128
STRIPS = 24
KSTEPS = 2
LAG = 4
PACKED = 264
WHOLE = 2
INSIDE = 4
PIECES = ((4, 8), (8, 11), (11, 14), (14, 16))


def half_of(value):
    return lax.rem(value, 2)


def kernel(a, out, blk, prv, awy, pkl, pkr, late, *refs):
    both, pieces, refs = refs[:WHOLE], refs[WHOLE:WHOLE + len(PIECES)], refs[WHOLE + len(PIECES):]
    work(a, out, blk, prv, awy, pkl, pkr, late, both, pieces, *refs)


def work(a, out, blk, prv, awy, pkl, pkr, late, both, pieces, res, stm, acc, fa, fb, fc, pk, fpa, fpb,
         s_x, r_x, s_d, r_d, s_y, r_y, s_r, r_r,
         l_res, l_stm, l_acc, l_fa, l_fb, l_st, l_tr, l_pk):
    m = lax.axis_index("m")
    y = lax.axis_index("kk")
    g = lax.axis_index("g")
    side = lax.div(g, 2)
    layers, rows, cols = a.shape
    kc = cols // KSTEPS
    n_strip = rows // TILE
    n_chunk = rows // CHUNK

    def at(start, size):
        return pl.ds(pl.multiple_of(start, size), size)

    def remote(src, dst, ss, rs, kk2, g2):
        return pltpu.make_async_remote_copy(src, dst, ss, rs, device_id=(m, kk2, g2), device_id_type=MESH)

    def enter(*peers):
        barrier = pltpu.get_barrier_semaphore()
        for peer in ((1 - y, g),) + peers:
            pl.semaphore_signal(barrier, inc=1, device_id=(m,) + peer, device_id_type=MESH)
        pl.semaphore_wait(barrier, 1 + len(peers))

    def x_in(c):
        part = half_of(g)
        return remote(a.at[1 - side, at(c * CHUNK, CHUNK)], blk.at[1 + part, at(c * CHUNK, CHUNK)],
                      s_x.at[c], r_x.at[part, c], y, 2 - side)

    def x_start(c, carry):
        x_in(c).start()
        return carry

    def x_wait_send(c, carry):
        x_in(c).wait_send()
        return carry

    def body_steps(res_view, acc_view, swap, before, after):
        acc_view[...] = jnp.zeros(acc_view.shape, F32)

        def step(k, carry):
            before(k)
            pltpu.make_async_copy(a.at[0, pl.ds(0, TILE), pl.ds(0, kc)], stm.at[k], l_stm.at[k]).wait()
            lhs = res_view[:, at(k * kc, kc)]
            rhs = stm[k]
            if swap:
                lhs, rhs = rhs, lhs
            acc_view[...] += lax.dot_general(lhs, rhs, NT, preferred_element_type=F32)
            after(k)
            return carry

        lax.fori_loop(0, KSTEPS, step, 0)

    def diagonal():
        d = lax.div(g, 3)
        mate = g + 1 - 2 * d
        d2d = remote(a.at[side], blk.at[0], s_d.at[0], r_d.at[0], y, mate)

        def phase(r):
            return lax.div(r, 8), lax.rem(lax.div(r, 4), 2), n_strip - 1 - lax.rem(r, 4)

        def count(r):
            p, _, i = phase(r)
            return (i + 1) + half_of(p) * (n_strip - 1 - i)

        def slot(p):
            return p * (1 - 2 * d) + 2 * d

        def load(own, layer, row, col, width, dst, sem):
            @pl.when(own)
            def _():
                pltpu.make_async_copy(a.at[layer, at(row, TILE), at(col, width)], dst, sem).start()

            @pl.when(jnp.logical_not(own))
            def _():
                pltpu.make_async_copy(blk.at[layer, at(row, TILE), at(col, width)], dst, sem).start()

        def load_res(r, k):
            p, layer, i = phase(r)
            own = p + 1 - d < 2
            load(own, layer, i * TILE, k * kc, kc, res.at[half_of(r), :, at(k * kc, kc)], l_res.at[half_of(r) * KSTEPS + k])

        def load_stm(r, j, k):
            p, layer, _ = phase(r)
            own = p + d < 2
            load(own, layer, j * TILE, k * kc, kc, stm.at[k], l_stm.at[k])

        def tile_of(ref, r, i, j):
            p, layer, _ = phase(r)
            return ref.at[slot(p), layer, at(i * TILE, TILE), at(j * TILE, TILE)]

        def is_diag(r, j):
            p, _, i = phase(r)
            return jnp.logical_and(p != 1, i == j)

        def is_mirror(r, j):
            p, _, i = phase(r)
            return jnp.logical_and(p != 1, i != j)

        def whole(r, j):
            i = phase(r)[2]
            return remote(tile_of(out, r, i, j), tile_of(prv, r, i, j),
                          s_y.at[lax.rem(r, 8) * 4 + j], r_y.at[r * 4 + j], 1 - y, g)

        def lower(r, j, row, height, width):
            p, layer, i = phase(r)

            def part(ref):
                return ref.at[slot(p), layer, pl.ds(pl.multiple_of(i * TILE + row, SQUARE), height), pl.ds(pl.multiple_of(j * TILE, TILE), width)]

            return remote(part(out), part(prv), s_y.at[lax.rem(r, 8) * 4 + j], r_y.at[r * 4 + j], 1 - y, g)

        def packed_no(r):
            return lax.rem(r, 8) + 8 * lax.div(phase(r)[0], 2)

        def packed(r):
            e = packed_no(r)
            return remote(pkl.at[e], pkr.at[e], s_y.at[32 + lax.rem(r, 8)], r_y.at[4 * STRIPS + e], 1 - y, g)

        def store_packed(r):
            return pltpu.make_async_copy(pk, pkl.at[packed_no(r)], l_pk.at[0])

        def load_packed(r):
            e = packed_no(r)
            return pltpu.make_async_copy(pkl.at[e], fpa, l_pk.at[1]), pltpu.make_async_copy(pkr.at[e], fpb, l_pk.at[2])

        row_id = lax.broadcasted_iota(jnp.int32, (SQUARE, SQUARE), 0)
        col_id = lax.broadcasted_iota(jnp.int32, (SQUARE, SQUARE), 1)

        def square(ref, k):
            span = pl.ds(SQUARE * k, SQUARE)
            return ref.at[span, span]

        def pack(tile):
            ends = []
            for h in range(2):
                first, second = square(tile, 2 * h)[...], square(tile, 2 * h + 1)[...]
                pk[pl.ds(SQUARE * h, SQUARE), :] = jnp.where(row_id > col_id, first, second.T)
                ends.append(jnp.sum(jnp.where(row_id == col_id, first, 0.0), axis=0, keepdims=True))
            pk[pl.ds(2 * SQUARE, 8), :] = jnp.where(row_id[:8] == 0, *ends)

        def unpack(tile):
            fpa[...] = fpa[...] + fpb[...]
            for h in range(2):
                shared = fpa[pl.ds(SQUARE * h, SQUARE), :]
                turned = shared.T
                ends = fpa[pl.ds(2 * SQUARE + h, 1), :]
                square(tile, 2 * h)[...] = jnp.where(row_id > col_id, shared, jnp.where(row_id == col_id, ends, turned))
                square(tile, 2 * h + 1)[...] = jnp.where(row_id <= col_id, shared, turned)

        def send(r, j):
            @pl.when(is_diag(r, j))
            def _():
                for row in range(SQUARE, TILE, SQUARE):
                    lower(r, j, row, SQUARE, row).start()
                store_packed(r).wait()
                packed(r).start()

            @pl.when(jnp.logical_not(is_diag(r, j)))
            def _():
                whole(r, j).start()

        def wait_exchange(r, j):
            @pl.when(is_diag(r, j))
            def _():
                sized = lower(r, j, 0, 3 * SQUARE // 2, TILE)
                sized.wait_send()
                sized.wait_recv()
                packed(r).wait_send()
                packed(r).wait_recv()

            @pl.when(jnp.logical_not(is_diag(r, j)))
            def _():
                whole(r, j).wait_send()
                whole(r, j).wait_recv()

        def store_acc(r, j):
            return pltpu.make_async_copy(acc.at[half_of(j)], tile_of(out, r, phase(r)[2], j), l_acc.at[half_of(j)])

        def finish(r):
            n = count(r)
            i = phase(r)[2]

            def loads(j):
                b = half_of(j)
                return (pltpu.make_async_copy(tile_of(out, r, i, j), fa.at[b], l_fa.at[b]),
                        pltpu.make_async_copy(tile_of(prv, r, i, j), fb.at[b], l_fb.at[b]))

            def start_loads(j):
                wait_exchange(r, j)
                for copy in loads(j):
                    copy.start()

                @pl.when(is_diag(r, j))
                def _():
                    for copy in load_packed(r):
                        copy.start()

            def main_store(j):
                return pltpu.make_async_copy(fa.at[half_of(j)], tile_of(out, r, i, j), l_st.at[half_of(j)])

            def mirror_store(j):
                return pltpu.make_async_copy(fc.at[half_of(j)], tile_of(out, r, j, i), l_tr.at[half_of(j)])

            def wait_stores(j):
                main_store(j).wait()

                @pl.when(is_mirror(r, j))
                def _():
                    mirror_store(j).wait()

            start_loads(0)

            def one(j, carry):
                b = half_of(j)

                @pl.when(j + 1 < n)
                def _():
                    @pl.when(j >= 1)
                    def _():
                        wait_stores(j - 1)

                    start_loads(j + 1)

                for copy in loads(j):
                    copy.wait()
                fa[b] = fa[b] + fb[b]

                @pl.when(is_mirror(r, j))
                def _():
                    fc[b] = fa[b].T
                    mirror_store(j).start()

                @pl.when(is_diag(r, j))
                def _():
                    total = fa[b]
                    at_row = lax.broadcasted_iota(jnp.int32, (TILE, TILE), 0)
                    at_col = lax.broadcasted_iota(jnp.int32, (TILE, TILE), 1)
                    fa[b] = jnp.where(at_row >= at_col, total, total.T)
                    for copy in load_packed(r):
                        copy.wait()
                    unpack(fa.at[b])

                main_store(j).start()
                return carry

            lax.fori_loop(0, n, one, 0)

            @pl.when(n >= 2)
            def _():
                wait_stores(n - 2)

            wait_stores(n - 1)

        load_res(0, 0)
        load_stm(0, 0, 0)
        enter((y, mate), (y, 2 - side))
        lax.fori_loop(0, n_chunk, x_start, 0)
        for k in range(1, KSTEPS):
            load_res(0, k)
            load_stm(0, 0, k)
        d2d.start()

        def strip(r, carry):
            @pl.when(r == 7)
            def _():
                remote(a.at[0], blk.at[0], s_d.at[0], r_d.at[0], y, mate).wait_recv()

            @pl.when(r == 11)
            def _():
                remote(a.at[1], blk.at[1], s_d.at[1], r_d.at[1], y, mate).wait_recv()

            @pl.when(jnp.logical_and(r >= 1, r + 1 < STRIPS))
            def _():
                for k in range(KSTEPS):
                    load_res(r + 1, k)

            n = count(r)

            def tile(j, carry):
                last = lax.div(j + 1, n)

                def before(k):
                    @pl.when(j == 0)
                    def _():
                        b = half_of(r)
                        pltpu.make_async_copy(a.at[0, pl.ds(0, TILE), pl.ds(0, kc)], res.at[b, :, pl.ds(0, kc)], l_res.at[b * KSTEPS + k]).wait()

                def after(k):
                    @pl.when(jnp.logical_and(r == 0, j == 0))
                    def _():
                        load_res(r + 1, k)

                    @pl.when(r + last < STRIPS)
                    def _():
                        load_stm(r + last, (j + 1) * (1 - last), k)

                    @pl.when(jnp.logical_and(k == 0, jnp.logical_and(j >= 1, r + j >= 2)))
                    def _():
                        store_acc(r, j - 1).wait()
                        send(r, j - 1)

                body_steps(res.at[half_of(r)], acc.at[half_of(j)], False, before, after)
                store_acc(r, j).start()

                @pl.when(is_diag(r, j))
                def _():
                    pack(acc.at[half_of(j)])
                    store_packed(r).start()

                @pl.when(jnp.logical_and(r == 0, j == 0))
                def _():
                    store_acc(r, j).wait()
                    send(r, j)

                return carry

            lax.fori_loop(0, n, tile, 0)
            store_acc(r, n - 1).wait()
            send(r, n - 1)

            @pl.when(r >= LAG)
            def _():
                finish(r - LAG)

            return carry

        lax.fori_loop(0, STRIPS, strip, 0)
        lax.fori_loop(STRIPS - LAG, STRIPS, lambda r, carry: (finish(r), carry)[1], 0)
        d2d.wait_send()
        lax.fori_loop(0, n_chunk, x_wait_send, 0)

    def cross(is_left):
        lc = 0 if is_left else 1
        mate = 0 if is_left else 3
        partner = 2 if is_left else 1
        enter((y, mate), (y, partner), (y, 3 - mate))
        lax.fori_loop(0, n_chunk, x_start, 0)
        for layer in range(layers):
            remote(a.at[layer], blk.at[layer], s_d.at[layer], r_d.at[layer], y, mate).start()

        remote(a.at[lc], blk.at[0], s_d.at[0], r_d.at[0], y, mate).wait_recv()

        def region(ref, rows_first, c):
            return ref.at[at(c * CHUNK, CHUNK), :] if rows_first else ref.at[:, at(c * CHUNK, CHUNK)]

        def piece(ref, c, q):
            if is_left:
                return ref.at[at(c * CHUNK, CHUNK), at(q * TILE, TILE)]
            return ref.at[at(q * TILE, TILE), at(c * CHUNK, CHUNK)]

        def block_of(half):
            return lax.rem(half + 1 - y + 2, 2)

        def kept(b):
            return lax.rem(b + 1 - y + 2, 2)

        def load_stm(t, k):
            half, js = lax.div(t, 4), lax.rem(t, 4)
            own = block_of(half) == 1 if is_left else half == 0

            @pl.when(own)
            def _():
                pltpu.make_async_copy(a.at[lc, at(js * TILE, TILE), at(k * kc, kc)], stm.at[k], l_stm.at[k]).start()

            @pl.when(jnp.logical_not(own))
            def _():
                pltpu.make_async_copy(blk.at[0, at(js * TILE, TILE), at(k * kc, kc)], stm.at[k], l_stm.at[k]).start()

        def res_copy(c, part):
            b = half_of(c)
            return pltpu.make_async_copy(blk.at[1 + part, at(c * CHUNK, CHUNK)], res.at[b, pl.ds(part * CHUNK, CHUNK)], l_fb.at[part])

        def acc_view(t):
            b = half_of(t)
            return acc.at[b, pl.ds(0, 2 * CHUNK), :] if is_left else acc.at[b, :, pl.ds(0, 2 * CHUNK)]

        def store_acc(c, t):
            b, half, js = half_of(t), lax.div(t, 4), lax.rem(t, 4)

            def views(q, dst):
                src = acc.at[b, pl.ds(q * CHUNK, CHUNK), :] if is_left else acc.at[b, :, pl.ds(q * CHUNK, CHUNK)]
                return pltpu.make_async_copy(src, piece(dst, c, js), l_acc.at[b * 2 + q])

            if is_left:
                return lambda op: (op(views(0, awy.at[half])), op(views(1, out.at[block_of(half), lc])))

            def both(op):
                @pl.when(half == 0)
                def _():
                    for q in range(2):
                        op(views(q, out.at[q, lc]))

                @pl.when(half == 1)
                def _():
                    for q in range(2):
                        op(views(q, awy.at[kept(q)]))

            return both

        def home(c, b):
            return remote(region(out.at[b, lc], is_left, c), region(prv.at[b, lc], is_left, c),
                          s_y.at[c * 2 + b], r_y.at[c * 2 + b], 1 - y, g)

        def spread(c):
            return remote(region(awy.at[0], is_left, c), region(prv.at[2, 0], is_left, c),
                          s_y.at[2 * n_chunk + c], r_y.at[2 * n_chunk + c], 1 - y, g)

        def away(c):
            return remote(region(awy.at[1], is_left, c), region(out.at[y, lc], is_left, c),
                          s_r.at[c], r_r.at[c], y, partner)

        def arrived(c):
            return remote(region(awy.at[1], not is_left, c), region(out.at[y, 1 - lc], not is_left, c),
                          s_r.at[c], r_r.at[c], y, partner)

        def away_late(c):
            return remote(pieces[0].at[c - INSIDE], late.at[c - INSIDE], s_r.at[c], r_r.at[c], y, partner)

        def gather_here(k):
            return remote(both[k].at[0], both[k].at[1], s_y.at[3 * n_chunk + k], r_y.at[3 * n_chunk + k], 1 - y, g)

        def gather(c, owner):
            here = region(out.at[owner, 1 - lc], not is_left, c)
            return remote(here, here, s_y.at[3 * n_chunk + c], r_y.at[3 * n_chunk + c], 1 - y, g)

        def add(c, local, received, store=None):
            def view(ref, q):
                return ref.at[0, pl.ds(q * CHUNK, CHUNK), :] if is_left else ref.at[0, :, pl.ds(q * CHUNK, CHUNK)]

            pairs = [(pltpu.make_async_copy(piece(local, c, q), view(fa, q), l_fa.at[q]),
                      pltpu.make_async_copy(piece(received, c, q), view(fb, q), l_fb.at[q])) for q in range(4)]
            for pair in pairs:
                for copy in pair:
                    copy.start()
            stores = [pltpu.make_async_copy(view(fa, q), piece(local, c, q), l_st.at[q]) for q in range(4)]
            for q in range(4):
                for copy in pairs[q]:
                    copy.wait()
                view(fa, q)[...] = view(fa, q)[...] + view(fb, q)[...]
                if store is None:
                    stores[q].start()
                else:
                    store(q, view(fa, q), stores[q])
            for q in range(4):
                stores[q].wait()

        def finish_away(c):
            spread(c).wait_recv()

            def store(q, total, inside):
                @pl.when(jnp.logical_and(c >= WHOLE, c < INSIDE))
                def _():
                    inside.start()

                def put(dst):
                    if is_left:
                        pltpu.make_async_copy(total, dst.at[:, pl.ds(q * TILE, TILE)], l_st.at[q]).start()
                    else:
                        for u in range(TILE // CHUNK):
                            pltpu.make_async_copy(total.at[pl.ds(u * CHUNK, CHUNK), :],
                                                  dst.at[:, pl.ds(q * TILE + u * CHUNK, CHUNK)], l_st.at[q]).start()

                for k in range(WHOLE):
                    @pl.when(c == k)
                    def _(k=k):
                        put(both[k].at[0])

                for (first, stop), piece_ref in zip(PIECES, pieces):
                    @pl.when(jnp.logical_and(c >= first, c < stop))
                    def _(first=first, piece_ref=piece_ref):
                        put(piece_ref.at[c - first])

            add(c, awy.at[1], prv.at[2, 0], store)

            for k in range(WHOLE):
                @pl.when(c == k)
                def _(k=k):
                    gather_here(k).start()

            @pl.when(jnp.logical_and(c >= WHOLE, c < INSIDE))
            def _():
                away(c).start()

            @pl.when(jnp.logical_and(c >= INSIDE, c < PIECES[0][1]))
            def _():
                away_late(c).start()

        def finish_home(c):
            for b in range(2):
                home(c, b).wait_send()
                home(c, b).wait_recv()
                add(c, out.at[b, lc], prv.at[b, lc])

        def forward(c):
            arrived(c).wait_recv()
            gather(c, y).start()

        for k in range(KSTEPS):
            load_stm(0, k)

        def compute(c):
            for part in range(2):
                remote(a.at[0, pl.ds(0, CHUNK)], blk.at[1 + part, at(c * CHUNK, CHUNK)], s_x.at[0], r_x.at[part, c], y, partner).wait_recv()
                res_copy(c, part).start()
            for part in range(2):
                res_copy(c, part).wait()

            def send_half(half):
                if is_left:
                    @pl.when(half == 0)
                    def _():
                        spread(c).start()

                    home(c, block_of(half)).start()
                else:
                    @pl.when(half == 0)
                    def _():
                        for b in range(2):
                            home(c, b).start()

                    @pl.when(half == 1)
                    def _():
                        spread(c).start()

            def tile(t, carry):
                last = lax.div(t + 1, 8)

                def after(k):
                    @pl.when(c + last < n_chunk)
                    def _():
                        load_stm((t + 1) * (1 - last), k)

                    @pl.when(jnp.logical_and(k == 0, t >= 1))
                    def _():
                        store_acc(c, t - 1)(lambda copy: copy.wait())

                        @pl.when(t == 4)
                        def _():
                            send_half(0 * t)

                        @pl.when(jnp.logical_and(c == n_chunk - 1, t == 2))
                        def _():
                            forward(WHOLE)

                body_steps(res.at[half_of(c), pl.ds(0, 2 * CHUNK), :], acc_view(t), not is_left, lambda k: None, after)
                store_acc(c, t)(lambda copy: copy.start())
                return carry

            lax.fori_loop(0, 8, tile, 0)
            store_acc(c, 7)(lambda copy: copy.wait())
            send_half(1 + 0 * c)

            @pl.when(c == n_chunk - 1)
            def _():
                for k in range(WHOLE + 1, INSIDE):
                    forward(k)

        early = n_chunk - 2

        def drain_early():
            lax.fori_loop(0, early, x_wait_send, 0)
            lax.fori_loop(0, early, drain_spread, 0)
            for layer in range(layers):
                remote(a.at[layer], blk.at[layer], s_d.at[layer], r_d.at[layer], y, mate).wait_send()
            for k in range(WHOLE):
                gather_here(k).wait_send()
                gather_here(k).wait_recv()

        def drain_spread(c, carry):
            spread(c).wait_send()
            return carry

        def chunk(c, carry):
            pl.when(c == n_chunk - 1)(drain_early)
            compute(c)

            @pl.when(c >= 1)
            def _():
                finish_away(c - 1)
                finish_home(c - 1)

            return carry

        lax.fori_loop(0, n_chunk, chunk, 0)
        finish_away(n_chunk - 1)
        finish_home(n_chunk - 1)

        def drain(c, carry):
            away(c).wait_send()
            gather(c, y).wait_send()
            gather(c, 1 - y).wait_recv()
            return carry

        lax.fori_loop(early, n_chunk, drain_spread, 0)
        lax.fori_loop(early, n_chunk, x_wait_send, 0)
        for c in range(*PIECES[0]):
            away_late(c).wait_send()
            away_late(c).wait_recv()
        lax.fori_loop(WHOLE, INSIDE, drain, 0)

    pl.when(lax.rem(g, 3) == 0)(diagonal)
    pl.when(g == 1)(lambda: cross(True))
    pl.when(g == 2)(lambda: cross(False))


def assembly(step, first, *refs):
    n_in = len(first) + (step <= 2)
    ins, (out, *scratch) = refs[:n_in], refs[n_in:]
    buf, wide, l_in, l_out, l_win, l_wout = scratch
    y = lax.axis_index("kk")
    g = lax.axis_index("g")
    depth = buf.shape[0]
    lead = depth // 2

    def at(start, size):
        return pl.ds(pl.multiple_of(start, size), size)

    def copies(n, where):
        src = ins[-1]

        def view(ref, t):
            slot, layer, i, j = where(t)
            return ref.at[slot, layer, at(i * TILE, TILE), at(j * TILE, TILE)]

        def load(t):
            b = lax.rem(t, depth)
            return pltpu.make_async_copy(view(src, t), buf.at[b], l_in.at[b])

        def store(t):
            b = lax.rem(t, depth)
            return pltpu.make_async_copy(buf.at[b], view(out, t), l_out.at[b])

        def one(t, carry):
            @pl.when(jnp.logical_and(t >= depth, t < n))
            def _():
                store(t - depth).wait()

            @pl.when(t < n)
            def _():
                load(t).start()

            @pl.when(t >= lead)
            def _():
                load(t - lead).wait()
                store(t - lead).start()

            return carry

        lax.fori_loop(0, n + lead, one, 0)

        def last(t, carry):
            store(t).wait()
            return carry

        lax.fori_loop(max(n - depth, 0), n, last, 0)

    def zeros():
        buf[0] = jnp.zeros((TILE, TILE), F32)

        def store(b, layer, t):
            return pltpu.make_async_copy(buf.at[0], out.at[2, layer, at(lax.div(t, 4) * TILE, TILE), at(lax.rem(t, 4) * TILE, TILE)], l_out.at[b])

        for layer in range(2):
            for t in range(16):
                store(t, layer, t).start()
            for t in range(16):
                store(t, layer, t).wait()

    def away_results(is_left):
        layer = 1 if is_left else 0
        todo = []
        for k, ranges in enumerate(first):
            chunks = [(c, slot) for span, slot in zip(ranges, (y, 1 - y)) if span for c in range(*span)]
            todo += [(k, c, n, slot) for n, (c, slot) in enumerate(chunks)]

        def load(t):
            k, _, n, _ = todo[t]
            return pltpu.make_async_copy(ins[k].at[n], wide.at[t], l_win.at[t])

        def whole(t):
            _, c, _, slot = todo[t]
            return pltpu.make_async_copy(wide.at[t], out.at[slot, layer, pl.ds(c * CHUNK, CHUNK), :], l_wout.at[t])

        for t in range(len(todo)):
            load(t).start()
        for t in range(len(todo)):
            k, c, _, slot = todo[t]
            load(t).wait()
            if not is_left:
                whole(t).start()
            else:
                for u in range(out.shape[2] // CHUNK):
                    pltpu.make_async_copy(wide.at[t, :, pl.ds(u * CHUNK, CHUNK)],
                                          out.at[slot, layer, pl.ds(u * CHUNK, CHUNK), pl.ds(c * CHUNK, CHUNK)], l_wout.at[t]).start()
        for t in range(len(todo)):
            whole(t).wait()

    def on_cross(is_left):
        lc = 0 if is_left else 1
        away_results(is_left)
        if step == 0:
            if is_left:
                copies(8, lambda t: (lax.div(t, 4), 1 - lc, lax.rem(t, 4), 0))
            else:
                copies(8, lambda t: (lax.div(t, 4), 1 - lc, 0, lax.rem(t, 4)))
        elif step <= 2:
            copies(16, lambda t: (step - 1, lc, lax.div(t, 4), lax.rem(t, 4)))
            if step == 2:
                zeros()

    @pl.when(g == 1)
    def _():
        on_cross(True)

    @pl.when(g == 2)
    def _():
        on_cross(False)

    if step < 3:
        @pl.when(lax.rem(g, 3) == 0)
        def _():
            copies(32, lambda t: (step, lax.div(t, 16), lax.div(lax.rem(t, 16), 4), lax.rem(t, 4)))


def solution(mesh):
    assert dict(mesh.shape) == {"m": 1, "kk": 2, "g": 4}
    dma = pltpu.SemaphoreType.DMA

    def local_part(a_loc):
        layers, rows, cols = a_loc.shape
        n_chunk = rows // CHUNK
        any_space = pl.BlockSpec(memory_space=pl.ANY)
        slots_shape = jax.ShapeDtypeStruct((3, layers, rows, rows), F32)

        def chunks_shape(n):
            return jax.ShapeDtypeStruct((n, CHUNK, rows), F32)

        slots, _, _, _, _, _, late, *others = pl.pallas_call(
            kernel,
            out_shape=(
                slots_shape,
                jax.ShapeDtypeStruct((3, rows, cols), a_loc.dtype),
                slots_shape,
                jax.ShapeDtypeStruct((2, rows, rows), F32),
                *(jax.ShapeDtypeStruct((16, PACKED, SQUARE), F32) for _ in range(2)),
                chunks_shape(PIECES[0][1] - PIECES[0][0]),
                *(chunks_shape(2) for _ in range(WHOLE)),
                *(chunks_shape(stop - start) for start, stop in PIECES),
            ),
            in_specs=[any_space],
            out_specs=(any_space,) * (7 + WHOLE + len(PIECES)),
            scratch_shapes=[
                pltpu.VMEM((2, TILE, cols), a_loc.dtype),
                pltpu.VMEM((KSTEPS, TILE, cols // KSTEPS), a_loc.dtype),
                *[pltpu.VMEM((2, TILE, TILE), F32)] * 4,
                *[pltpu.VMEM((PACKED, SQUARE), F32)] * 3,
                dma((n_chunk,)), dma((2, n_chunk)), dma((2,)), dma((2,)),
                dma((4 * n_chunk,)), dma((4 * STRIPS + 16,)), dma((n_chunk,)), dma((n_chunk,)),
                dma((2 * KSTEPS,)), dma((KSTEPS,)), *[dma((4,))] * 6,
            ],
            compiler_params=pltpu.CompilerParams(
                collective_id=0, has_side_effects=True, vmem_limit_bytes=63 * 2**20),
            cost_estimate=pl.CostEstimate(flops=10**12, bytes_accessed=10**9, transcendentals=0),
        )(a_loc)

        both, pieces = others[:WHOLE], others[WHOLE:]
        other_chip = [(1, 2), (2, 1)]
        other_half = [(1, 5), (5, 1), (2, 6), (6, 2)]

        n_pieces = len(PIECES)
        mine = [late] + [lax.ppermute(pieces[k], "g", other_chip) for k in range(1, n_pieces)]
        theirs = [lax.ppermute(mine[k], ("kk", "g"), other_half) for k in range(n_pieces)]
        pairs = [lax.ppermute(both[k], "g", other_chip) for k in range(WHOLE)]

        def assemble(step, result, parts):
            first = tuple(((k, k + 1),) * 2 if kind == "pair" else (PIECES[k], None) if kind == "mine" else (None, PIECES[k])
                          for kind, k in parts)
            arrays = [{"mine": mine, "theirs": theirs, "pair": pairs}[kind][k] for kind, k in parts]
            n_wide = max(1, sum(stop - start for ranges in first for start, stop in filter(None, ranges)))
            sources = arrays + ([slots] if step <= 2 else [])
            aliases = {}
            operands = sources
            if step > 0:
                operands = [result] + sources
                aliases = {0: 0}

            def body(*refs):
                assembly(step, first, *refs[len(operands) - len(sources):])

            return pl.pallas_call(
                body,
                out_shape=slots_shape,
                in_specs=[any_space] * len(operands),
                out_specs=any_space,
                input_output_aliases=aliases,
                scratch_shapes=[
                    pltpu.VMEM((16, TILE, TILE), F32), pltpu.VMEM((n_wide, CHUNK, rows), F32),
                    dma((16,)), dma((16,)), dma((n_wide,)), dma((n_wide,)),
                ],
                compiler_params=pltpu.CompilerParams(vmem_limit_bytes=67043328),
                cost_estimate=pl.CostEstimate(flops=10**10, bytes_accessed=10**8, transcendentals=0),
            )(*operands)

        result = assemble(0, None, [])
        for step in range(1, n_pieces + WHOLE + 1):
            own, other = step - 1, step - WHOLE - 1
            parts = [("mine", own) if own < n_pieces else ("pair", own - n_pieces)]
            result = assemble(step, result, parts + ([("theirs", other)] if other >= 0 else []))
        return result[None]

    return jax.shard_map(local_part, mesh=mesh, in_specs=(P(None, ("m", "g"), "kk"),),
                         out_specs=P(("m", "g"), None, None, None, None), check_vma=False)
```

```python
import jax
import jax.numpy as jnp
from jax import lax
from jax.experimental import pallas as pl
from jax.experimental.pallas import tpu as pltpu
from jax.sharding import PartitionSpec as P


MESH = pl.DeviceIdType.MESH
NT = (((1,), (1,)), ((), ()))
F32 = jnp.float32

SQUARE = 128
TILE = 512
CHUNK = 128
STRIPS = 24
KSTEPS = 2
LAG = 4
PACKED = 264
QUARTERS = 4
AHEAD = (4, 3)
WHOLE = len(AHEAD)
INSIDE = 4
INNER = tuple((c, q) for c in range(INSIDE) for q in range((AHEAD + (0,) * INSIDE)[c], QUARTERS))
HOOKS = 8
PIECES = ((4, 8), (8, 11), (11, 13), (13, 15), (15, 16))


def half_of(value):
    return lax.rem(value, 2)


def kernel(a, out, blk, prv, awy, pkl, pkr, late, *refs):
    both, pieces, refs = refs[:WHOLE], refs[WHOLE:WHOLE + len(PIECES)], refs[WHOLE + len(PIECES):]
    work(a, out, blk, prv, awy, pkl, pkr, late, both, pieces, *refs)


def work(a, out, blk, prv, awy, pkl, pkr, late, both, pieces, res, stm, acc, fa, fb, fc, pk, fpa, fpb,
         s_x, r_x, s_d, r_d, s_y, r_y, s_r, r_r,
         l_res, l_stm, l_acc, l_fa, l_fb, l_st, l_tr, l_pk):
    m = lax.axis_index("m")
    y = lax.axis_index("kk")
    g = lax.axis_index("g")
    side = lax.div(g, 2)
    layers, rows, cols = a.shape
    kc = cols // KSTEPS
    n_strip = rows // TILE
    n_chunk = rows // CHUNK

    def at(start, size):
        return pl.ds(pl.multiple_of(start, size), size)

    def remote(src, dst, ss, rs, kk2, g2):
        return pltpu.make_async_remote_copy(src, dst, ss, rs, device_id=(m, kk2, g2), device_id_type=MESH)

    def enter(*peers):
        barrier = pltpu.get_barrier_semaphore()
        for peer in ((1 - y, g),) + peers:
            pl.semaphore_signal(barrier, inc=1, device_id=(m,) + peer, device_id_type=MESH)
        pl.semaphore_wait(barrier, 1 + len(peers))

    def x_in(c):
        part = half_of(g)
        return remote(a.at[1 - side, at(c * CHUNK, CHUNK)], blk.at[1 + part, at(c * CHUNK, CHUNK)],
                      s_x.at[c], r_x.at[part, c], y, 2 - side)

    def x_start(c, carry):
        x_in(c).start()
        return carry

    def x_wait_send(c, carry):
        x_in(c).wait_send()
        return carry

    def body_steps(res_view, acc_view, swap, before, after):
        acc_view[...] = jnp.zeros(acc_view.shape, F32)

        def step(k, carry):
            before(k)
            pltpu.make_async_copy(a.at[0, pl.ds(0, TILE), pl.ds(0, kc)], stm.at[k], l_stm.at[k]).wait()
            lhs = res_view[:, at(k * kc, kc)]
            rhs = stm[k]
            if swap:
                lhs, rhs = rhs, lhs
            acc_view[...] += lax.dot_general(lhs, rhs, NT, preferred_element_type=F32)
            after(k)
            return carry

        lax.fori_loop(0, KSTEPS, step, 0)

    def diagonal():
        d = lax.div(g, 3)
        mate = g + 1 - 2 * d
        d2d = remote(a.at[side], blk.at[0], s_d.at[0], r_d.at[0], y, mate)

        def phase(r):
            return lax.div(r, 8), lax.rem(lax.div(r, 4), 2), n_strip - 1 - lax.rem(r, 4)

        def count(r):
            p, _, i = phase(r)
            return (i + 1) + half_of(p) * (n_strip - 1 - i)

        def slot(p):
            return p * (1 - 2 * d) + 2 * d

        def load(own, layer, row, col, width, dst, sem):
            @pl.when(own)
            def _():
                pltpu.make_async_copy(a.at[layer, at(row, TILE), at(col, width)], dst, sem).start()

            @pl.when(jnp.logical_not(own))
            def _():
                pltpu.make_async_copy(blk.at[layer, at(row, TILE), at(col, width)], dst, sem).start()

        def load_res(r, k):
            p, layer, i = phase(r)
            own = p + 1 - d < 2
            load(own, layer, i * TILE, k * kc, kc, res.at[half_of(r), :, at(k * kc, kc)], l_res.at[half_of(r) * KSTEPS + k])

        def load_stm(r, j, k):
            p, layer, _ = phase(r)
            own = p + d < 2
            load(own, layer, j * TILE, k * kc, kc, stm.at[k], l_stm.at[k])

        def tile_of(ref, r, i, j):
            p, layer, _ = phase(r)
            return ref.at[slot(p), layer, at(i * TILE, TILE), at(j * TILE, TILE)]

        def is_diag(r, j):
            p, _, i = phase(r)
            return jnp.logical_and(p != 1, i == j)

        def is_mirror(r, j):
            p, _, i = phase(r)
            return jnp.logical_and(p != 1, i != j)

        def whole(r, j):
            i = phase(r)[2]
            return remote(tile_of(out, r, i, j), tile_of(prv, r, i, j),
                          s_y.at[lax.rem(r, 8) * 4 + j], r_y.at[r * 4 + j], 1 - y, g)

        def lower(r, j, row, height, width):
            p, layer, i = phase(r)

            def part(ref):
                return ref.at[slot(p), layer, pl.ds(pl.multiple_of(i * TILE + row, SQUARE), height), pl.ds(pl.multiple_of(j * TILE, TILE), width)]

            return remote(part(out), part(prv), s_y.at[lax.rem(r, 8) * 4 + j], r_y.at[r * 4 + j], 1 - y, g)

        def packed_no(r):
            return lax.rem(r, 8) + 8 * lax.div(phase(r)[0], 2)

        def packed(r):
            e = packed_no(r)
            return remote(pkl.at[e], pkr.at[e], s_y.at[32 + lax.rem(r, 8)], r_y.at[4 * STRIPS + e], 1 - y, g)

        def store_packed(r):
            return pltpu.make_async_copy(pk, pkl.at[packed_no(r)], l_pk.at[0])

        def load_packed(r):
            e = packed_no(r)
            return pltpu.make_async_copy(pkl.at[e], fpa, l_pk.at[1]), pltpu.make_async_copy(pkr.at[e], fpb, l_pk.at[2])

        row_id = lax.broadcasted_iota(jnp.int32, (SQUARE, SQUARE), 0)
        col_id = lax.broadcasted_iota(jnp.int32, (SQUARE, SQUARE), 1)

        def square(ref, k):
            span = pl.ds(SQUARE * k, SQUARE)
            return ref.at[span, span]

        def pack(tile):
            ends = []
            for h in range(2):
                first, second = square(tile, 2 * h)[...], square(tile, 2 * h + 1)[...]
                pk[pl.ds(SQUARE * h, SQUARE), :] = jnp.where(row_id > col_id, first, second.T)
                ends.append(jnp.sum(jnp.where(row_id == col_id, first, 0.0), axis=0, keepdims=True))
            pk[pl.ds(2 * SQUARE, 8), :] = jnp.where(row_id[:8] == 0, *ends)

        def unpack(tile):
            fpa[...] = fpa[...] + fpb[...]
            for h in range(2):
                shared = fpa[pl.ds(SQUARE * h, SQUARE), :]
                turned = shared.T
                ends = fpa[pl.ds(2 * SQUARE + h, 1), :]
                square(tile, 2 * h)[...] = jnp.where(row_id > col_id, shared, jnp.where(row_id == col_id, ends, turned))
                square(tile, 2 * h + 1)[...] = jnp.where(row_id <= col_id, shared, turned)

        def send(r, j):
            @pl.when(is_diag(r, j))
            def _():
                for row in range(SQUARE, TILE, SQUARE):
                    lower(r, j, row, SQUARE, row).start()
                store_packed(r).wait()
                packed(r).start()

            @pl.when(jnp.logical_not(is_diag(r, j)))
            def _():
                whole(r, j).start()

        def wait_exchange(r, j):
            @pl.when(is_diag(r, j))
            def _():
                sized = lower(r, j, 0, 3 * SQUARE // 2, TILE)
                sized.wait_send()
                sized.wait_recv()
                packed(r).wait_send()
                packed(r).wait_recv()

            @pl.when(jnp.logical_not(is_diag(r, j)))
            def _():
                whole(r, j).wait_send()
                whole(r, j).wait_recv()

        def store_acc(r, j):
            return pltpu.make_async_copy(acc.at[half_of(j)], tile_of(out, r, phase(r)[2], j), l_acc.at[half_of(j)])

        def finish(r):
            n = count(r)
            i = phase(r)[2]

            def loads(j):
                b = half_of(j)
                return (pltpu.make_async_copy(tile_of(out, r, i, j), fa.at[b], l_fa.at[b]),
                        pltpu.make_async_copy(tile_of(prv, r, i, j), fb.at[b], l_fb.at[b]))

            def start_loads(j):
                wait_exchange(r, j)
                for copy in loads(j):
                    copy.start()

                @pl.when(is_diag(r, j))
                def _():
                    for copy in load_packed(r):
                        copy.start()

            def main_store(j):
                return pltpu.make_async_copy(fa.at[half_of(j)], tile_of(out, r, i, j), l_st.at[half_of(j)])

            def mirror_store(j):
                return pltpu.make_async_copy(fc.at[half_of(j)], tile_of(out, r, j, i), l_tr.at[half_of(j)])

            def wait_stores(j):
                main_store(j).wait()

                @pl.when(is_mirror(r, j))
                def _():
                    mirror_store(j).wait()

            start_loads(0)

            def one(j, carry):
                b = half_of(j)

                @pl.when(j + 1 < n)
                def _():
                    @pl.when(j >= 1)
                    def _():
                        wait_stores(j - 1)

                    start_loads(j + 1)

                for copy in loads(j):
                    copy.wait()
                fa[b] = fa[b] + fb[b]

                @pl.when(is_mirror(r, j))
                def _():
                    fc[b] = fa[b].T
                    mirror_store(j).start()

                @pl.when(is_diag(r, j))
                def _():
                    total = fa[b]
                    at_row = lax.broadcasted_iota(jnp.int32, (TILE, TILE), 0)
                    at_col = lax.broadcasted_iota(jnp.int32, (TILE, TILE), 1)
                    fa[b] = jnp.where(at_row >= at_col, total, total.T)
                    for copy in load_packed(r):
                        copy.wait()
                    unpack(fa.at[b])

                main_store(j).start()
                return carry

            lax.fori_loop(0, n, one, 0)

            @pl.when(n >= 2)
            def _():
                wait_stores(n - 2)

            wait_stores(n - 1)

        load_res(0, 0)
        load_stm(0, 0, 0)
        enter((y, mate), (y, 2 - side))
        lax.fori_loop(0, n_chunk, x_start, 0)
        for k in range(1, KSTEPS):
            load_res(0, k)
            load_stm(0, 0, k)
        d2d.start()

        def strip(r, carry):
            @pl.when(r == 7)
            def _():
                remote(a.at[0], blk.at[0], s_d.at[0], r_d.at[0], y, mate).wait_recv()

            @pl.when(r == 11)
            def _():
                remote(a.at[1], blk.at[1], s_d.at[1], r_d.at[1], y, mate).wait_recv()

            @pl.when(jnp.logical_and(r >= 1, r + 1 < STRIPS))
            def _():
                for k in range(KSTEPS):
                    load_res(r + 1, k)

            n = count(r)

            def tile(j, carry):
                last = lax.div(j + 1, n)

                def before(k):
                    @pl.when(j == 0)
                    def _():
                        b = half_of(r)
                        pltpu.make_async_copy(a.at[0, pl.ds(0, TILE), pl.ds(0, kc)], res.at[b, :, pl.ds(0, kc)], l_res.at[b * KSTEPS + k]).wait()

                def after(k):
                    @pl.when(jnp.logical_and(r == 0, j == 0))
                    def _():
                        load_res(r + 1, k)

                    @pl.when(r + last < STRIPS)
                    def _():
                        load_stm(r + last, (j + 1) * (1 - last), k)

                    @pl.when(jnp.logical_and(k == 0, jnp.logical_and(j >= 1, r + j >= 2)))
                    def _():
                        store_acc(r, j - 1).wait()
                        send(r, j - 1)

                body_steps(res.at[half_of(r)], acc.at[half_of(j)], False, before, after)
                store_acc(r, j).start()

                @pl.when(is_diag(r, j))
                def _():
                    pack(acc.at[half_of(j)])
                    store_packed(r).start()

                @pl.when(jnp.logical_and(r == 0, j == 0))
                def _():
                    store_acc(r, j).wait()
                    send(r, j)

                return carry

            lax.fori_loop(0, n, tile, 0)
            store_acc(r, n - 1).wait()
            send(r, n - 1)

            @pl.when(r >= LAG)
            def _():
                finish(r - LAG)

            return carry

        lax.fori_loop(0, STRIPS, strip, 0)
        lax.fori_loop(STRIPS - LAG, STRIPS, lambda r, carry: (finish(r), carry)[1], 0)
        d2d.wait_send()
        lax.fori_loop(0, n_chunk, x_wait_send, 0)

    def cross(is_left):
        lc = 0 if is_left else 1
        mate = 0 if is_left else 3
        partner = 2 if is_left else 1
        enter((y, mate), (y, partner), (y, 3 - mate))
        lax.fori_loop(0, n_chunk, x_start, 0)
        for layer in range(layers):
            remote(a.at[layer], blk.at[layer], s_d.at[layer], r_d.at[layer], y, mate).start()

        remote(a.at[lc], blk.at[0], s_d.at[0], r_d.at[0], y, mate).wait_recv()

        def region(ref, rows_first, c):
            return ref.at[at(c * CHUNK, CHUNK), :] if rows_first else ref.at[:, at(c * CHUNK, CHUNK)]

        def piece(ref, c, q):
            if is_left:
                return ref.at[at(c * CHUNK, CHUNK), at(q * TILE, TILE)]
            return ref.at[at(q * TILE, TILE), at(c * CHUNK, CHUNK)]

        def turned_piece(ref, c, q):
            if is_left:
                return ref.at[at(q * TILE, TILE), at(c * CHUNK, CHUNK)]
            return ref.at[at(c * CHUNK, CHUNK), at(q * TILE, TILE)]

        def block_of(half):
            return lax.rem(half + 1 - y + 2, 2)

        def kept(b):
            return lax.rem(b + 1 - y + 2, 2)

        def load_stm(t, k):
            half, js = lax.div(t, 4), lax.rem(t, 4)
            own = block_of(half) == 1 if is_left else half == 0

            @pl.when(own)
            def _():
                pltpu.make_async_copy(a.at[lc, at(js * TILE, TILE), at(k * kc, kc)], stm.at[k], l_stm.at[k]).start()

            @pl.when(jnp.logical_not(own))
            def _():
                pltpu.make_async_copy(blk.at[0, at(js * TILE, TILE), at(k * kc, kc)], stm.at[k], l_stm.at[k]).start()

        def res_copy(c, part):
            b = half_of(c)
            return pltpu.make_async_copy(blk.at[1 + part, at(c * CHUNK, CHUNK)], res.at[b, pl.ds(part * CHUNK, CHUNK)], l_fb.at[part])

        def acc_view(t):
            b = half_of(t)
            return acc.at[b, pl.ds(0, 2 * CHUNK), :] if is_left else acc.at[b, :, pl.ds(0, 2 * CHUNK)]

        def store_acc(c, t):
            b, half, js = half_of(t), lax.div(t, 4), lax.rem(t, 4)

            def views(q, dst):
                src = acc.at[b, pl.ds(q * CHUNK, CHUNK), :] if is_left else acc.at[b, :, pl.ds(q * CHUNK, CHUNK)]
                return pltpu.make_async_copy(src, piece(dst, c, js), l_acc.at[b * 2 + q])

            if is_left:
                return lambda op: (op(views(0, awy.at[half])), op(views(1, out.at[block_of(half), lc])))

            def both(op):
                @pl.when(half == 0)
                def _():
                    for q in range(2):
                        op(views(q, out.at[q, lc]))

                @pl.when(half == 1)
                def _():
                    for q in range(2):
                        op(views(q, awy.at[kept(q)]))

            return both

        def home(c, b):
            return remote(region(out.at[b, lc], is_left, c), region(prv.at[b, lc], is_left, c),
                          s_y.at[c * 2 + b], r_y.at[c * 2 + b], 1 - y, g)

        def spread(c):
            return remote(region(awy.at[0], is_left, c), region(prv.at[2, 0], is_left, c),
                          s_y.at[2 * n_chunk + c], r_y.at[2 * n_chunk + c], 1 - y, g)

        def away(h):
            return remote(piece(awy.at[1], *INNER[h]), piece(out.at[y, lc], *INNER[h]), s_r.at[h], r_r.at[h], y, partner)

        def arrived(h):
            return remote(turned_piece(awy.at[1], *INNER[h]), turned_piece(out.at[y, 1 - lc], *INNER[h]),
                          s_r.at[h], r_r.at[h], y, partner)

        def away_late(c):
            n = c - INSIDE + len(INNER)
            return remote(pieces[0].at[c - INSIDE], late.at[c - INSIDE], s_r.at[n], r_r.at[n], y, partner)

        def gather_here(k):
            n = 3 * n_chunk + len(INNER) + k
            return remote(both[k].at[0], both[k].at[1], s_y.at[n], r_y.at[n], 1 - y, g)

        def gather(h, owner):
            here = turned_piece(out.at[owner, 1 - lc], *INNER[h])
            return remote(here, here, s_y.at[3 * n_chunk + h], r_y.at[3 * n_chunk + h], 1 - y, g)

        def add(c, local, received, store=None):
            def view(ref, q):
                return ref.at[0, pl.ds(q * CHUNK, CHUNK), :] if is_left else ref.at[0, :, pl.ds(q * CHUNK, CHUNK)]

            pairs = [(pltpu.make_async_copy(piece(local, c, q), view(fa, q), l_fa.at[q]),
                      pltpu.make_async_copy(piece(received, c, q), view(fb, q), l_fb.at[q])) for q in range(4)]
            for pair in pairs:
                for copy in pair:
                    copy.start()
            stores = [pltpu.make_async_copy(view(fa, q), piece(local, c, q), l_st.at[q]) for q in range(4)]
            for q in range(4):
                for copy in pairs[q]:
                    copy.wait()
                view(fa, q)[...] = view(fa, q)[...] + view(fb, q)[...]
                if store is None:
                    stores[q].start()
                else:
                    store(q, view(fa, q), stores[q])
            for q in range(4):
                stores[q].wait()

        def finish_away(c):
            spread(c).wait_recv()

            def store(q, total, inside):
                for k in range(INSIDE):
                    if (k, q) in INNER:
                        pl.when(c == k)(inside.start)

                def put(dst):
                    if is_left:
                        pltpu.make_async_copy(total, dst.at[:, pl.ds(q * TILE, TILE)], l_st.at[q]).start()
                    else:
                        for u in range(TILE // CHUNK):
                            pltpu.make_async_copy(total.at[pl.ds(u * CHUNK, CHUNK), :],
                                                  dst.at[:, pl.ds(q * TILE + u * CHUNK, CHUNK)], l_st.at[q]).start()

                for k in range(WHOLE):
                    if q < AHEAD[k]:
                        @pl.when(c == k)
                        def _(k=k):
                            put(both[k].at[0])

                for (first, stop), piece_ref in zip(PIECES, pieces):
                    @pl.when(jnp.logical_and(c >= first, c < stop))
                    def _(first=first, piece_ref=piece_ref):
                        put(piece_ref.at[c - first])

            add(c, awy.at[1], prv.at[2, 0], store)

            for k in range(INSIDE):
                @pl.when(c == k)
                def _(k=k):
                    if k < WHOLE:
                        gather_here(k).start()
                    for h, (chunk, _) in enumerate(INNER):
                        if chunk == k:
                            away(h).start()

            @pl.when(jnp.logical_and(c >= INSIDE, c < PIECES[0][1]))
            def _():
                away_late(c).start()

        def finish_home(c):
            for b in range(2):
                home(c, b).wait_send()
                home(c, b).wait_recv()
                add(c, out.at[b, lc], prv.at[b, lc])

        def forward(h):
            arrived(h).wait_recv()
            gather(h, y).start()

        for k in range(KSTEPS):
            load_stm(0, k)

        def compute(c):
            for part in range(2):
                remote(a.at[0, pl.ds(0, CHUNK)], blk.at[1 + part, at(c * CHUNK, CHUNK)], s_x.at[0], r_x.at[part, c], y, partner).wait_recv()
                res_copy(c, part).start()
            for part in range(2):
                res_copy(c, part).wait()

            def send_half(half):
                if is_left:
                    @pl.when(half == 0)
                    def _():
                        spread(c).start()

                    home(c, block_of(half)).start()
                else:
                    @pl.when(half == 0)
                    def _():
                        for b in range(2):
                            home(c, b).start()

                    @pl.when(half == 1)
                    def _():
                        spread(c).start()

            def tile(t, carry):
                last = lax.div(t + 1, 8)

                def after(k):
                    for h in range(HOOKS):
                        @pl.when(jnp.logical_and(c == n_chunk - 1, t * KSTEPS + k == h))
                        def _(h=h):
                            forward(h)

                    @pl.when(c + last < n_chunk)
                    def _():
                        load_stm((t + 1) * (1 - last), k)

                    @pl.when(jnp.logical_and(k == 0, t >= 1))
                    def _():
                        store_acc(c, t - 1)(lambda copy: copy.wait())

                        @pl.when(t == 4)
                        def _():
                            send_half(0 * t)


                body_steps(res.at[half_of(c), pl.ds(0, 2 * CHUNK), :], acc_view(t), not is_left, lambda k: None, after)
                store_acc(c, t)(lambda copy: copy.start())
                return carry

            lax.fori_loop(0, 8, tile, 0)
            store_acc(c, 7)(lambda copy: copy.wait())
            send_half(1 + 0 * c)

            @pl.when(c == n_chunk - 1)
            def _():
                for h in range(HOOKS, len(INNER)):
                    forward(h)

        early = n_chunk - 2

        def drain_early():
            lax.fori_loop(0, early, x_wait_send, 0)
            lax.fori_loop(0, early, drain_spread, 0)
            for layer in range(layers):
                remote(a.at[layer], blk.at[layer], s_d.at[layer], r_d.at[layer], y, mate).wait_send()
            for k in range(WHOLE):
                gather_here(k).wait_send()
                gather_here(k).wait_recv()

        def drain_spread(c, carry):
            spread(c).wait_send()
            return carry

        def chunk(c, carry):
            pl.when(c == n_chunk - 1)(drain_early)
            compute(c)

            @pl.when(c >= 1)
            def _():
                finish_away(c - 1)
                finish_home(c - 1)

            return carry

        lax.fori_loop(0, n_chunk, chunk, 0)
        finish_away(n_chunk - 1)
        finish_home(n_chunk - 1)

        lax.fori_loop(early, n_chunk, drain_spread, 0)
        lax.fori_loop(early, n_chunk, x_wait_send, 0)
        for c in range(*PIECES[0]):
            away_late(c).wait_send()
            away_late(c).wait_recv()
        for h in range(len(INNER)):
            away(h).wait_send()
            gather(h, y).wait_send()
            gather(h, 1 - y).wait_recv()

    pl.when(lax.rem(g, 3) == 0)(diagonal)
    pl.when(g == 1)(lambda: cross(True))
    pl.when(g == 2)(lambda: cross(False))


def assembly(step, first, *refs):
    n_in = len(first) + (step <= 2)
    ins, (out, *scratch) = refs[:n_in], refs[n_in:]
    buf, wide, l_in, l_out, l_win, l_wout = scratch
    y = lax.axis_index("kk")
    g = lax.axis_index("g")
    depth = buf.shape[0]
    lead = depth // 2

    def at(start, size):
        return pl.ds(pl.multiple_of(start, size), size)

    def copies(n, where):
        src = ins[-1]

        def view(ref, t):
            slot, layer, i, j = where(t)
            return ref.at[slot, layer, at(i * TILE, TILE), at(j * TILE, TILE)]

        def load(t):
            b = lax.rem(t, depth)
            return pltpu.make_async_copy(view(src, t), buf.at[b], l_in.at[b])

        def store(t):
            b = lax.rem(t, depth)
            return pltpu.make_async_copy(buf.at[b], view(out, t), l_out.at[b])

        def one(t, carry):
            @pl.when(jnp.logical_and(t >= depth, t < n))
            def _():
                store(t - depth).wait()

            @pl.when(t < n)
            def _():
                load(t).start()

            @pl.when(t >= lead)
            def _():
                load(t - lead).wait()
                store(t - lead).start()

            return carry

        lax.fori_loop(0, n + lead, one, 0)

        def last(t, carry):
            store(t).wait()
            return carry

        lax.fori_loop(max(n - depth, 0), n, last, 0)

    def zeros():
        buf[0] = jnp.zeros((TILE, TILE), F32)

        def store(b, layer, t):
            return pltpu.make_async_copy(buf.at[0], out.at[2, layer, at(lax.div(t, 4) * TILE, TILE), at(lax.rem(t, 4) * TILE, TILE)], l_out.at[b])

        for layer in range(2):
            for t in range(16):
                store(t, layer, t).start()
            for t in range(16):
                store(t, layer, t).wait()

    def away_results(is_left):
        layer = 1 if is_left else 0
        todo = []
        for k, ranges in enumerate(first):
            chunks = [(c, slot) for span, slot in zip(ranges, (y, 1 - y)) if span for c in range(*span)]
            todo += [(k, c, n, slot) for n, (c, slot) in enumerate(chunks)]

        def load(t):
            k, _, n, _ = todo[t]
            return pltpu.make_async_copy(ins[k].at[n], wide.at[t, :, pl.ds(0, ins[k].shape[-1])], l_win.at[t])

        def whole(t):
            k, c, _, slot = todo[t]
            span = pl.ds(0, ins[k].shape[-1])
            return pltpu.make_async_copy(wide.at[t, :, span], out.at[slot, layer, pl.ds(c * CHUNK, CHUNK), span], l_wout.at[t])

        for t in range(len(todo)):
            load(t).start()
        for t in range(len(todo)):
            k, c, _, slot = todo[t]
            load(t).wait()
            if not is_left:
                whole(t).start()
            else:
                for u in range(ins[k].shape[-1] // CHUNK):
                    pltpu.make_async_copy(wide.at[t, :, pl.ds(u * CHUNK, CHUNK)],
                                          out.at[slot, layer, pl.ds(u * CHUNK, CHUNK), pl.ds(c * CHUNK, CHUNK)], l_wout.at[t]).start()
        for t in range(len(todo)):
            whole(t).wait()

    def on_cross(is_left):
        lc = 0 if is_left else 1
        away_results(is_left)
        if step == 0:
            if is_left:
                copies(8, lambda t: (lax.div(t, 4), 1 - lc, lax.rem(t, 4), 0))
            else:
                copies(8, lambda t: (lax.div(t, 4), 1 - lc, 0, lax.rem(t, 4)))
        elif step <= 2:
            copies(16, lambda t: (step - 1, lc, lax.div(t, 4), lax.rem(t, 4)))
            if step == 2:
                zeros()

    @pl.when(g == 1)
    def _():
        on_cross(True)

    @pl.when(g == 2)
    def _():
        on_cross(False)

    if step < 3:
        @pl.when(lax.rem(g, 3) == 0)
        def _():
            copies(32, lambda t: (step, lax.div(t, 16), lax.div(lax.rem(t, 16), 4), lax.rem(t, 4)))


def solution(mesh):
    assert dict(mesh.shape) == {"m": 1, "kk": 2, "g": 4}
    dma = pltpu.SemaphoreType.DMA

    def local_part(a_loc):
        layers, rows, cols = a_loc.shape
        n_chunk = rows // CHUNK
        any_space = pl.BlockSpec(memory_space=pl.ANY)
        slots_shape = jax.ShapeDtypeStruct((3, layers, rows, rows), F32)

        def chunks_shape(n):
            return jax.ShapeDtypeStruct((n, CHUNK, rows), F32)

        slots, _, _, _, _, _, late, *others = pl.pallas_call(
            kernel,
            out_shape=(
                slots_shape,
                jax.ShapeDtypeStruct((3, rows, cols), a_loc.dtype),
                slots_shape,
                jax.ShapeDtypeStruct((2, rows, rows), F32),
                *(jax.ShapeDtypeStruct((16, PACKED, SQUARE), F32) for _ in range(2)),
                chunks_shape(PIECES[0][1] - PIECES[0][0]),
                *(jax.ShapeDtypeStruct((2, CHUNK, n * TILE), F32) for n in AHEAD),
                *(chunks_shape(stop - start) for start, stop in PIECES),
            ),
            in_specs=[any_space],
            out_specs=(any_space,) * (7 + WHOLE + len(PIECES)),
            scratch_shapes=[
                pltpu.VMEM((2, TILE, cols), a_loc.dtype),
                pltpu.VMEM((KSTEPS, TILE, cols // KSTEPS), a_loc.dtype),
                *[pltpu.VMEM((2, TILE, TILE), F32)] * 4,
                *[pltpu.VMEM((PACKED, SQUARE), F32)] * 3,
                dma((n_chunk,)), dma((2, n_chunk)), dma((2,)), dma((2,)),
                dma((4 * n_chunk,)), dma((4 * STRIPS + 16,)), dma((n_chunk,)), dma((n_chunk,)),
                dma((2 * KSTEPS,)), dma((KSTEPS,)), *[dma((4,))] * 6,
            ],
            compiler_params=pltpu.CompilerParams(
                collective_id=0, has_side_effects=True, vmem_limit_bytes=63 * 2**20),
            cost_estimate=pl.CostEstimate(flops=10**12, bytes_accessed=10**9, transcendentals=0),
        )(a_loc)

        both, pieces = others[:WHOLE], others[WHOLE:]
        other_chip = [(1, 2), (2, 1)]
        other_half = [(1, 5), (5, 1), (2, 6), (6, 2)]

        n_pieces = len(PIECES)
        mine = [late] + [lax.ppermute(pieces[k], "g", other_chip) for k in range(1, n_pieces)]
        theirs = [lax.ppermute(mine[k], ("kk", "g"), other_half) for k in range(n_pieces)]
        pairs = [lax.ppermute(both[k], "g", other_chip) for k in range(WHOLE)]

        def assemble(step, result, parts):
            first = tuple(((k, k + 1),) * 2 if kind == "pair" else (PIECES[k], None) if kind == "mine" else (None, PIECES[k])
                          for kind, k in parts)
            arrays = [{"mine": mine, "theirs": theirs, "pair": pairs}[kind][k] for kind, k in parts]
            n_wide = max(1, sum(stop - start for ranges in first for start, stop in filter(None, ranges)))
            sources = arrays + ([slots] if step <= 2 else [])
            aliases = {}
            operands = sources
            if step > 0:
                operands = [result] + sources
                aliases = {0: 0}

            def body(*refs):
                assembly(step, first, *refs[len(operands) - len(sources):])

            return pl.pallas_call(
                body,
                out_shape=slots_shape,
                in_specs=[any_space] * len(operands),
                out_specs=any_space,
                input_output_aliases=aliases,
                scratch_shapes=[
                    pltpu.VMEM((16, TILE, TILE), F32), pltpu.VMEM((n_wide, CHUNK, rows), F32),
                    dma((16,)), dma((16,)), dma((n_wide,)), dma((n_wide,)),
                ],
                compiler_params=pltpu.CompilerParams(vmem_limit_bytes=67043328),
                cost_estimate=pl.CostEstimate(flops=10**10, bytes_accessed=10**8, transcendentals=0),
            )(*operands)

        result = assemble(0, None, [])
        for step in range(1, n_pieces + WHOLE + 1):
            own, other = step - 1, step - WHOLE - 1
            parts = [("mine", own) if own < n_pieces else ("pair", own - n_pieces)]
            result = assemble(step, result, parts + ([("theirs", other)] if other >= 0 else []))
        return result[None]

    return jax.shard_map(local_part, mesh=mesh, in_specs=(P(None, ("m", "g"), "kk"),),
                         out_specs=P(("m", "g"), None, None, None, None), check_vma=False)
```
